128 devices in a mesh: pb: 4 (over y), db: 32 (over z, x, core).
Axes of the slice: x: 4, y: 4, z: 4, core: 2. Of those that a mesh axis runs over, the one named last changes fastest.
Arguments:
- slab: float32 [262144, 1024], P('db', 'pb'), may hold values from -6 to 6
- queries: float32 [512, 1024], P('db', 'pb'), may hold values from -6 to 6
- block_ids: int32 [512, 16], P('db'), may hold values from 0 to 16383, as said below
Outputs:
- scores: float32 [512, 256], P('db')
- gram: float32 [512, 256, 256], P('db', 'pb')
- penalty: float32 [512, 256, 256], P('db', 'pb')
The draws below stay inside these ranges and needn't reach their ends.
Inputs may be any that keep to these rules, and one draw needn't show every extreme that they name: `block_ids`: block id k lies in the slab rows of db index k // 512. Among the ids of the 16 queries of one db index, no db index is named more than 12 times, and one db index, the same for all db indices, is named exactly 12 times.
All inputs are finite; a program needn't handle non-finite values.
Results may differ from the reference program's by a relative error of at most 0.000096.
Values sent between devices are 32-bit elements; how exact they have to be, the bound alone decides.
A program may use at most 128 MiB of HBM per device.

```python
import math
import jax
import jax.numpy as jnp
import numpy as np
from jax import lax

W = 1024
BLOCK = 16
NQB = 16
SLAB_DEV = 8192
Q_COL = 16
CAND = 256
ROWS = 262144
QUERIES = 512
N_DB = 32


def draw_block_ids(key, part):
    request_count = Q_COL * NQB
    capacity = 3 * request_count // (2 * N_DB)
    rest_ranks = np.repeat(np.arange(1, N_DB), capacity).astype(np.int32)
    key_popular, key_devices = jax.random.split(jax.random.fold_in(key, 7))
    popular = jax.random.permutation(key_popular, N_DB).astype(jnp.int32)
    blocks_each = SLAB_DEV // BLOCK

    def per_device(device_key):
        key_one, key_two, key_three = jax.random.split(device_key, 3)
        shuffled = jax.random.permutation(key_one, jnp.asarray(rest_ranks, jnp.int32))
        ranks = jnp.concatenate([jnp.zeros((capacity,), jnp.int32), shuffled[:request_count - capacity]])
        ranks = jax.random.permutation(key_two, ranks)
        owners = popular[ranks]
        local_block = jax.random.randint(key_three, (request_count,), 0, blocks_each).astype(jnp.int32)
        return (owners * blocks_each + local_block).reshape(Q_COL, NQB)
    device_keys = jax.random.split(key_devices, N_DB)
    return jax.vmap(per_device)(device_keys).reshape(Q_COL * N_DB, NQB).astype(jnp.int32)


def levels(stream_key, shape, cuts, least, top_value):
    def one(axis_at, blocks):
        steps = jax.random.uniform(jax.random.fold_in(jax.random.fold_in(stream_key, 6), axis_at), (blocks,), jnp.float32, least / len(cuts), top_value / len(cuts))
        return jnp.repeat(jnp.exp(steps), shape[axis_at] // blocks).reshape((-1,) + (1,) * (len(shape) - axis_at - 1))

    factor_of = one(*cuts[0])
    for cut in cuts[1:]:
        factor_of = factor_of * one(*cut)
    return factor_of


def normal_values(own_key, shape, deviation, limit, shards=(), kind=jnp.bfloat16):
    result = deviation * jax.random.normal(own_key, shape, jnp.float32)
    if shards:
        result = result * levels(own_key, shape, shards, -0.22, 0.18)
    return jnp.clip(result, -limit, limit).astype(kind)


def setup_inputs(seed: int = 0) -> dict:
    key_list = jax.random.split(jax.random.key(seed), 4)
    slab = normal_values(key_list[0], (ROWS, W), 1.0, 6.0, ((0, 32), (1, 4)), jnp.float32)
    queries = normal_values(key_list[1], (QUERIES, W), 1.0, 6.0, ((0, 32), (1, 4)), jnp.float32)
    block_ids = draw_block_ids(jax.random.fold_in(key_list[3], 71), 0)
    return dict(slab=slab, queries=queries, block_ids=block_ids)


epsilon = 1e-06

def reference(slab, queries, block_ids):
    slab_blocks = slab.reshape(-1, BLOCK, W)
    highest = lax.Precision.HIGHEST

    def per_query(pair):
        query_vec, query_ids = pair
        cand_rows = slab_blocks[query_ids].reshape(CAND, W)
        query_norm = jnp.sqrt(jnp.sum(query_vec * query_vec) + epsilon)
        row_norm = jnp.sqrt(lax.optimization_barrier(jnp.sum(cand_rows * cand_rows, axis=1)) + epsilon)
        query_dots = jnp.dot(cand_rows, query_vec, precision=highest)
        score_row = math.sqrt(W) * query_dots / (query_norm * row_norm)
        raw_gram = jnp.dot(cand_rows, cand_rows.T, precision=highest)
        gram_mat = raw_gram / (row_norm[:, None] * row_norm[None, :])
        penalty_mat = gram_mat * jax.nn.sigmoid(score_row[None, :] - score_row[:, None])
        return (score_row, gram_mat, penalty_mat)
    scores, gram, penalty = lax.map(per_query, (queries, block_ids))
    return (scores, gram, penalty)
```

```python
import functools
import math

import jax
import jax.numpy as jnp
from jax import lax
from jax.experimental import pallas as pl
from jax.experimental.pallas import tpu as pltpu
from jax.sharding import PartitionSpec as P

BLOCK = 16
CAP = 12
HALF = 6
NZ, NX, NC, NY = 4, 4, 2, 4
EPS = 1e-06
MESH = pl.DeviceIdType.MESH
F32 = jnp.float32
CHUNKS = ((0, 0), (1, 0), (0, 1), (1, 1))
NCH = len(CHUNKS)
WIDE = [(d, e) for d in range(4) for e in range(2) if (d, e) != (0, 0)]


def main_kernel(scale, tab, pos, query, slab, gram_out, score_out, slabv, tmid, tfin, tsm, src_a, mid_a, src_b, mid_b,
                fin0, fin1, fin2, fin3, ysend, cand, qall, acc, sq, dt, grecv, srecv, gsend, ssend,
                lsem, tsem, ts1, tr1, ts2, tr2, s1s, s1r, s2s, s2r, ys, yr, qs, qr, gs, gr, ss, sr):
    fin = (fin0, fin1, fin2, fin3)
    y = lax.axis_index("pb")
    db = lax.axis_index("db")
    z, x, c = db // (NX * NC), (db // NC) % NX, db % NC
    jx = x * NC + c
    jz = z * NC + c

    def dev(yy, zz, xx, cc):
        return (yy, (zz * NX + xx) * NC + cc)

    def up(v, d, n):
        return (v + d) % n

    load = pltpu.make_async_copy(slab, slabv, lsem)
    load.start()

    peers = [dev(y, up(z, d, NZ), x, up(c, e, NC)) for d, e in WIDE]
    peers += [dev(y, z, up(x, d, NX), up(c, e, NC)) for d, e in WIDE if d]
    peers += [dev(up(y, d, NY), z, x, c) for d in range(1, NY)]
    barrier = pltpu.get_barrier_semaphore()
    for p in peers:
        pl.semaphore_signal(barrier, inc=1, device_id=p, device_id_type=MESH)
    pl.semaphore_wait(barrier, len(peers))

    sends = []

    def remote(src, dst, ssem, rsem, target):
        cp = pltpu.make_async_remote_copy(src_ref=src, dst_ref=dst, send_sem=ssem, recv_sem=rsem,
                                          device_id=target, device_id_type=MESH)
        cp.start()
        sends.append(cp)
        return cp

    first = [remote(tab.at[up(z, d, NZ)], tmid.at[z], ts1.at[d - 1], tr1.at[d - 1], dev(y, up(z, d, NZ), x, c))
             for d in range(1, NZ)]
    qcopies = [remote(query.at[up(y, d, NY)], qall.at[y], qs.at[d - 1], qr.at[d - 1], dev(up(y, d, NY), z, x, c))
               for d in range(1, NY)]
    qall[y] = query[y]
    tmid[z] = tab[z]
    for cp in first:
        cp.wait_recv()
    second = []
    for k, (d, e) in enumerate(WIDE):
        x2, c2 = up(x, d, NX), up(c, e, NC)
        second.append(remote(tmid.at[:, x2 * NC + c2], tfin.at[jx], ts2.at[k], tr2.at[k], dev(y, z, x2, c2)))
    tfin[jx] = tmid[:, jx]
    for cp in second:
        cp.wait_recv()
    tcopy = pltpu.make_async_copy(tfin, tsm, tsem)
    tcopy.start()
    tcopy.wait()
    load.wait()

    def gather(ch):
        h, f = CHUNKS[ch]
        rows, lanes = slice(8 * h, 8 * h + 8), slice(128 * f, 128 * f + 128)

        for d in range(4):
            z2, x2 = up(z, d, NZ), up(x, d, NX)

            def body(j, carry):
                to_a = mid_a if d == 0 else src_a
                to_b = mid_b if d == 0 else src_b
                for s in range(HALF):
                    to_a[ch, z2, j, s] = slabv[tsm[j, z2, 0, s], rows, lanes]
                for s in range(HALF):
                    to_b[ch, x2, j, s] = slabv[tsm[x2 * NC + j % NC, j // NC, 0, HALF + s], rows, lanes]
                return carry

            lax.fori_loop(0, 8, body, 0)

    def stage1(ch):
        cps = []
        for d in range(1, 4):
            z2, x2 = up(z, d, NZ), up(x, d, NX)
            cps.append(remote(src_a.at[ch, z2], mid_a.at[ch, z], s1s.at[ch, 0, d - 1], s1r.at[ch, 0, d - 1], dev(y, z2, x, c)))
            cps.append(remote(src_b.at[ch, x2], mid_b.at[ch, x], s1s.at[ch, 1, d - 1], s1r.at[ch, 1, d - 1], dev(y, z, x2, c)))
        return cps

    def stage2(ch, before):
        for cp in before:
            cp.wait_recv()
        cps = []
        for k, (d, e) in enumerate(WIDE):
            z2, x2, c2 = up(z, d, NZ), up(x, d, NX), up(c, e, NC)
            cps.append(remote(mid_a.at[ch, :, x2 * NC + c2], fin[ch].at[:, c, x, 0:HALF], s2s.at[ch, 0, k], s2r.at[ch, 0, k], dev(y, z, x2, c2)))
            cps.append(remote(mid_b.at[ch, :, z2 * NC + c2], fin[ch].at[z, c, :, HALF:CAP], s2s.at[ch, 1, k], s2r.at[ch, 1, k], dev(y, z2, x, c2)))
        for i in range(4):
            fin[ch][i, c, x, 0:HALF] = mid_a[ch, i, jx]
            fin[ch][z, c, i, HALF:CAP] = mid_b[ch, i, jz]
        return cps

    def across(ch, before):
        h, f = CHUNKS[ch]
        for cp in before:
            cp.wait_recv()
        cps = []
        for d in (1, 3, 2, 0):
            y2 = up(y, d, NY)

            def body(i, carry):
                for u in range(8):
                    t = i * 8 + u
                    r = y2 * 64 + t
                    val = fin[ch][pos[0, r], pos[1, r], pos[2, r], pos[3, r]]
                    if d:
                        ysend[ch, d - 1, t] = val
                    else:
                        cand[y, f, t, h] = val
                return carry

            lax.fori_loop(0, 8, body, 0)
            if d:
                cps.append(remote(ysend.at[ch, d - 1], cand.at[y, f, :, h], ys.at[ch, d - 1], yr.at[ch, d - 1], dev(y2, z, x, c)))
        return cps

    def nt(a, b):
        return lax.dot_general(a, b, (((1,), (1,)), ((), ())), preferred_element_type=F32)

    def partial(q, f):
        s2 = jnp.zeros((256, 128), F32)
        dd = jnp.zeros((256, 128), F32)
        g = jnp.zeros((256, 256), F32)
        for yp in range(0, NY, 2):
            his, los = [], []
            for yy in (yp, yp + 1):
                v = cand[yy, f, pl.ds(q * 16, 16)].reshape(256, 128)
                qv = qall[yy, q, :, 128 * f:128 * f + 128]
                s2 = s2 + v * v
                dd = dd + v * qv
                hi = v.astype(jnp.bfloat16)
                his.append(hi)
                los.append((v - hi.astype(F32)).astype(jnp.bfloat16))
            hi = jnp.concatenate(his, axis=1)
            lo = jnp.concatenate(los, axis=1)
            g = g + (nt(hi, hi) + (nt(hi, lo) + nt(lo, hi)))
        return g, s2, dd

    def first_half(q, carry):
        g, s2, dd = partial(q, 0)
        acc[q] = g
        sq[q] = s2
        dt[q] = dd
        return carry

    gather(0)
    a0 = stage1(0)
    gather(1)
    a1 = stage1(1)
    gather(2)
    b0 = stage2(0, a0)
    a2 = stage1(2)
    gather(3)
    b1 = stage2(1, a1)
    a3 = stage1(3)
    c0 = across(0, b0)
    b2 = stage2(2, a2)
    c1 = across(1, b1)
    b3 = stage2(3, a3)
    c2 = across(2, b2)
    for cp in qcopies:
        cp.wait_recv()
    for cp in c0 + c1:
        cp.wait_recv()
    lax.fori_loop(0, 4, first_half, 0)
    c3 = across(3, b3)
    for cp in c2 + c3:
        cp.wait_recv()

    lane = lax.broadcasted_iota(jnp.int32, (256, 128), 1)
    outs = []
    for q in range(4):
        g, s2, dd = partial(q, 1)
        g = g + acc[q]
        rn = 1.0 / jnp.sqrt(jnp.sum(s2 + sq[q], axis=1, keepdims=True) + EPS)
        dots = jnp.sum(dd + dt[q], axis=1, keepdims=True)
        qsum = jnp.zeros((1, 128), F32)
        for yy in range(NY):
            for f in range(2):
                qv = qall[yy, q, :, 128 * f:128 * f + 128]
                qsum = qsum + qv * qv
        qn = jnp.sqrt(jnp.sum(qsum, axis=1, keepdims=True) + EPS)
        score = (scale * dots) * (rn / qn)
        both = jnp.where(lane == 0, rn, score)
        flat = both.T
        gsend[q] = g * rn * flat[0:1, :]
        ssend[q] = flat[1:2, :]
        for d in (1, 3, 2):
            y2 = up(y, d, NY)
            outs.append(remote(gsend.at[q, pl.ds(y2 * 64, 64)], grecv.at[y * 4 + q], gs.at[q, d - 1], gr.at[q, d - 1], dev(y2, z, x, c)))
            outs.append(remote(ssend.at[q], srecv.at[y * 4 + q], ss.at[q, d - 1], sr.at[q, d - 1], dev(y2, z, x, c)))
        grecv[y * 4 + q] = gsend[q, pl.ds(pl.multiple_of(y * 64, 64), 64)]
        srecv[y * 4 + q] = ssend[q]
    for cp in outs:
        cp.wait_recv()
    gram_out[...] = grecv[...]
    score_out[...] = srecv[...]
    for cp in sends:
        cp.wait_send()


def main_call(scale, tab, pos, query, slab):
    dma = pltpu.SemaphoreType.DMA
    vm = pltpu.VMEM
    vmem = pl.BlockSpec(memory_space=pltpu.VMEM)
    return pl.pallas_call(
        functools.partial(main_kernel, scale),
        out_shape=(jax.ShapeDtypeStruct((16, 64, 256), F32), jax.ShapeDtypeStruct((16, 1, 256), F32)),
        in_specs=[vmem, pl.BlockSpec(memory_space=pltpu.SMEM), vmem, pl.BlockSpec(memory_space=pl.ANY)],
        out_specs=(vmem, vmem),
        scratch_shapes=[
            vm(slab.shape, F32),
            vm((4, 8, 1, 128), jnp.int32), vm((8, 4, 1, 128), jnp.int32), pltpu.SMEM((8, 4, 1, 128), jnp.int32),
            vm((NCH, 4, 8, HALF, 8, 128), F32), vm((NCH, 4, 8, HALF, 8, 128), F32),
            vm((NCH, 4, 8, HALF, 8, 128), F32), vm((NCH, 4, 8, HALF, 8, 128), F32),
            *[vm((NZ, NC, NX, CAP, 8, 128), F32) for _ in range(NCH)],
            vm((NCH, 3, 64, 8, 128), F32), vm((NY, 2, 64, 2, 8, 128), F32), vm((NY, 4, 1, 256), F32),
            vm((4, 256, 256), F32), vm((4, 256, 128), F32), vm((4, 256, 128), F32),
            vm((16, 64, 256), F32), vm((16, 1, 256), F32), vm((4, 256, 256), F32), vm((4, 1, 256), F32),
            dma(()), dma(()), dma((3,)), dma((3,)), dma((7,)), dma((7,)),
            dma((NCH, 2, 3)), dma((NCH, 2, 3)), dma((NCH, 2, 7)), dma((NCH, 2, 7)),
            dma((NCH, 3)), dma((NCH, 3)), dma((3,)), dma((3,)), dma((4, 3)), dma((4, 3)), dma((4, 3)), dma((4, 3)),
        ],
        compiler_params=pltpu.CompilerParams(collective_id=0, has_side_effects=True, vmem_limit_bytes=60 * 2**20),
    )(tab, pos, query, slab)


def per_device(slab, queries, block_ids):
    query_count, width_part = queries.shape
    db_count = lax.axis_size("db")
    pb_count = lax.axis_size("pb")
    full_width = width_part * pb_count
    blocks_named = block_ids.shape[1]
    blocks_each = slab.shape[0] // BLOCK
    request_count = query_count * blocks_named
    ids = block_ids.reshape(request_count)
    owner = ids // blocks_each
    local = ids % blocks_each
    k = jnp.arange(request_count, dtype=jnp.int32)
    earlier = (owner[:, None] == owner[None, :]) & (k[None, :] < k[:, None])
    slot = jnp.sum(earlier.astype(jnp.int32), axis=1)
    place = owner * 16 + slot
    wanted = jnp.arange(db_count * 16, dtype=jnp.int32)
    table = jnp.sum(jnp.where(place[None, :] == wanted[:, None], local[None, :], 0), axis=1)
    table = jnp.pad(table.reshape(db_count, 16), ((0, 0), (0, 112))).reshape(NZ, NX * NC, 1, 128)
    pos = jnp.stack([owner // 8, owner % 2, (owner // 2) % 4, slot])
    gram, scores = main_call(math.sqrt(full_width), table, pos, queries.reshape(pb_count, query_count // pb_count, 1, width_part),
                             slab.reshape(blocks_each, BLOCK, width_part))
    scores = scores.reshape(query_count, -1)
    own = lax.dynamic_slice_in_dim(scores, lax.axis_index("pb") * 64, 64, 1)
    penalty = gram * jax.nn.sigmoid(scores[:, None, :] - own[:, :, None])
    return (scores, gram, penalty)


def solution(mesh):
    return jax.shard_map(
        per_device,
        mesh=mesh,
        in_specs=(P("db", "pb"), P("db", "pb"), P("db", None)),
        out_specs=(P("db", None), P("db", "pb", None), P("db", "pb", None)),
        check_vma=False,
    )
```

```python
import functools
import math

import jax
import jax.numpy as jnp
from jax import lax
from jax.experimental import pallas as pl
from jax.experimental.pallas import tpu as pltpu
from jax.sharding import PartitionSpec as P

BLOCK = 16
CAP = 12
HALF = 6
NZ, NX, NC, NY = 4, 4, 2, 4
EPS = 1e-06
MESH = pl.DeviceIdType.MESH
F32 = jnp.float32
CHUNKS = ((8, 0, 0), (8, 8, 0), (4, 0, 1), (4, 4, 1), (4, 0, 2), (4, 4, 2))
NCH = len(CHUNKS)
STEPS = ((1, 0), (1, 1), (2, 0), (1, 2), (2, 1), (1, 3), (3, 0), (2, 2), (1, 4), (3, 1), (2, 3), (1, 5), (3, 2), ("wait", 0), ("wait", 1),
         ("sum", 0, 0), ("sum", 0, 1), (2, 4), ("sum", 0, 2), ("sum", 0, 3), (3, 3), (2, 5), ("wait", 2), ("wait", 3),
         ("sum", 1, 0), ("sum", 1, 1), ("sum", 1, 2), ("sum", 1, 3), (3, 4), (3, 5))
WIDE = [(d, e) for d in range(4) for e in range(2) if (d, e) != (0, 0)]


def main_kernel(scale, ids, query, slab, part_out, vec_out, slabv, idv, qall, qrow, tab, tmid, tfin, tsm, pos, psm, *rest):
    src_a, mid_a, src_b, mid_b, fin, ysend, cand = (rest[i * NCH:(i + 1) * NCH] for i in range(7))
    (acc, sq, dt, gsend, ssend,
     lsem, isem, psem, tsem, qsem, ts1, tr1, ts2, tr2, s1s, s1r, s2s, s2r, ys, yr, zs, zr, qs, qr, gs, gr, ss, sr) = rest[7 * NCH:]
    y = lax.axis_index("pb")
    db = lax.axis_index("db")
    z, x, c = db // (NX * NC), (db // NC) % NX, db % NC
    jx = x * NC + c
    jz = z * NC + c

    def dev(yy, zz, xx, cc):
        return (yy, (zz * NX + xx) * NC + cc)

    def up(v, d, n):
        return (v + d) % n

    peers = [dev(y, up(z, d, NZ), x, up(c, e, NC)) for d, e in WIDE]
    peers += [dev(y, z, up(x, d, NX), up(c, e, NC)) for d, e in WIDE if d]
    peers += [dev(up(y, d, NY), z, x, c) for d in range(1, NY)]
    barrier = pltpu.get_barrier_semaphore()
    for p in peers:
        pl.semaphore_signal(barrier, inc=1, device_id=p, device_id_type=MESH)
    icopy = pltpu.make_async_copy(ids, idv, isem)
    icopy.start()
    qcopy = pltpu.make_async_copy(query, qall.at[y], qsem)
    qcopy.start()
    load = pltpu.make_async_copy(slab, slabv, lsem)
    load.start()

    icopy.wait()
    wide = jnp.concatenate([idv[...]] * 8, axis=1)
    sub = lax.broadcasted_iota(jnp.int32, (16, 128), 0)
    lan = lax.broadcasted_iota(jnp.int32, (16, 128), 1)
    wide = jnp.where(lan // 16 == sub % 8, wide, 0)
    row = [jnp.sum(wide[8 * i:8 * i + 8], axis=0, keepdims=True) for i in range(2)]
    big_r = lax.broadcasted_iota(jnp.int32, (128, 128), 0)
    big_c = lax.broadcasted_iota(jnp.int32, (128, 128), 1)

    def column(v):
        return jnp.broadcast_to(v, (128, 128)).T

    each = slab.shape[0]
    own = [v // each for v in row]
    own_t = [column(v) for v in own]
    rank = [jnp.sum(jnp.where((own_t[0] == own[0]) & (big_r < big_c), 1, 0), axis=0, keepdims=True),
            jnp.sum(jnp.where(own_t[0] == own[1], 1, 0), axis=0, keepdims=True)
            + jnp.sum(jnp.where((own_t[1] == own[1]) & (big_r < big_c), 1, 0), axis=0, keepdims=True)]
    code_t = [column((own[i] * 16 + rank[i]) * each + row[i] % each) for i in range(2)]
    for zz in range(NZ):
        tab[zz] = sum(jnp.sum(jnp.where(code_t[i] // each == big_c + 128 * zz, code_t[i] % each, 0), axis=0, keepdims=True)
                      for i in range(2))
    for i in range(2):
        o = own[i]
        pos[i] = (((o // 8) * NC + o % 2) * NX + (o // 2) % 4) * CAP + rank[i]
    pcopy = pltpu.make_async_copy(pos, psm, psem)
    pcopy.start()
    tmid[z] = tab[z]

    pl.semaphore_wait(barrier, len(peers))
    sends = []

    def remote(src, dst, ssem, rsem, target):
        cp = pltpu.make_async_remote_copy(src_ref=src, dst_ref=dst, send_sem=ssem, recv_sem=rsem,
                                          device_id=target, device_id_type=MESH)
        cp.start()
        sends.append(cp)
        return cp

    first = [remote(tab.at[up(z, d, NZ)], tmid.at[z], ts1.at[d - 1], tr1.at[d - 1], dev(y, up(z, d, NZ), x, c))
             for d in range(1, NZ)]
    qcopy.wait()
    qcopies = [remote(qall.at[y], qall.at[y], qs.at[d - 1], qr.at[d - 1], dev(up(y, d, NY), z, x, c)) for d in range(1, NY)]
    for cp in first:
        cp.wait_recv()
    second = []
    for k, (d, e) in enumerate(WIDE):
        second.append(remote(tmid, tfin.at[jx], ts2.at[k], tr2.at[k], dev(y, z, up(x, d, NX), up(c, e, NC))))
    tfin[jx] = tmid[...]
    for cp in second:
        cp.wait_recv()
    tcopy = pltpu.make_async_copy(tfin, tsm, tsem)
    tcopy.start()
    load.wait()
    pcopy.wait()
    tcopy.wait()

    def tile(ch, at):
        n, r0, kind = CHUNKS[ch]
        if kind == 0:
            return slabv[at, r0:r0 + n, 0:128]
        top = slabv[at, r0:r0 + n, 128:256]
        low = slabv[at, 8 + r0:8 + r0 + n, 128:256]
        left = lax.broadcasted_iota(jnp.int32, (n, 128), 1) < 64
        if kind == 1:
            return jnp.where(left, top, pltpu.roll(low, 64, 1))
        return jnp.where(left, pltpu.roll(top, 64, 1), low)

    def gather(ch):
        for d in range(4):
            z2, x2 = up(z, d, NZ), up(x, d, NX)
            to_a = mid_a[ch] if d == 0 else src_a[ch]
            to_b = mid_b[ch] if d == 0 else src_b[ch]

            def body(j, carry):
                for s in range(HALF):
                    to_a[z2, j, s] = tile(ch, tsm[j, z2, 0, jx * 16 + s])
                for s in range(HALF):
                    to_b[x2, j, s] = tile(ch, tsm[x2 * NC + j % NC, j // NC, 0, jx * 16 + HALF + s])
                return carry

            lax.fori_loop(0, 8, body, 0)

    def stage1(ch):
        gather(ch)
        cps = []
        for d in (1, 3, 2):
            z2, x2 = up(z, d, NZ), up(x, d, NX)
            cps.append(remote(src_a[ch].at[z2], mid_a[ch].at[z], s1s.at[ch, 0, d - 1], s1r.at[ch, 0, d - 1], dev(y, z2, x, c)))
            cps.append(remote(src_b[ch].at[x2], mid_b[ch].at[x], s1s.at[ch, 1, d - 1], s1r.at[ch, 1, d - 1], dev(y, z, x2, c)))
        return cps

    def stage2(ch, before):
        for cp in before:
            cp.wait_recv()
        cps = []
        for k, (d, e) in enumerate(WIDE):
            z2, x2, c2 = up(z, d, NZ), up(x, d, NX), up(c, e, NC)
            cps.append(remote(mid_a[ch].at[:, x2 * NC + c2], fin[ch].at[:, c, x, 0:HALF], s2s.at[ch, 0, k], s2r.at[ch, 0, k], dev(y, z, x2, c2)))
            cps.append(remote(mid_b[ch].at[:, z2 * NC + c2], fin[ch].at[z, c, :, HALF:CAP], s2s.at[ch, 1, k], s2r.at[ch, 1, k], dev(y, z2, x, c2)))
        for i in range(4):
            fin[ch][i, c, x, 0:HALF] = mid_a[ch][i, jx]
            fin[ch][z, c, i, HALF:CAP] = mid_b[ch][i, jz]
        return cps

    def pick(ch, y2, q, out):
        flat = fin[ch].reshape(NZ * NC * NX * CAP, CHUNKS[ch][0], 128)
        upper = y2 // 2
        base = (y2 % 2) * 64 + q * 16
        for u in range(16):
            out[q * 16 + u] = flat[psm[upper, 0, base + u]]

    def across(ch, before):
        for cp in before:
            cp.wait_recv()
        cps = []
        for d in (1, 3, 2, 0):
            y2 = up(y, d, NY)
            out = ysend[ch].at[d - 1] if d else cand[ch].at[y]

            def body(q, carry):
                pick(ch, y2, q, out)
                return carry

            lax.fori_loop(0, 4, body, 0)
            if d:
                cps.append(remote(out, cand[ch].at[y], ys.at[ch, d - 1], yr.at[ch, d - 1], dev(y2, z, x, c)))
        return cps

    def across_last(ch, before):
        for cp in before:
            cp.wait_recv()
        cps = []
        for q in range(4):
            for d in (1, 3, 2, 0):
                y2 = up(y, d, NY)
                out = ysend[ch].at[d - 1] if d else cand[ch].at[y]
                pick(ch, y2, q, out)
                if d:
                    mine = pl.ds(q * 16, 16)
                    cps.append(remote(out.at[mine], cand[ch].at[y, mine], zs.at[q, d - 1], zr.at[q, d - 1], dev(y2, z, x, c)))
        return cps

    def nt(a, b):
        return lax.dot_general(a, b, (((1,), (1,)), ((), ())), preferred_element_type=F32)

    left16 = lax.broadcasted_iota(jnp.int32, (16, 8, 128), 2) < 64

    def swap(v):
        return pltpu.roll(v, 64, v.ndim - 1)

    def operands(q, kind):
        mine = pl.ds(q * 16, 16)
        if kind == 0:
            return [jnp.stack([cand[0][yy, mine], cand[1][yy, mine]], axis=1).reshape(256, 128) for yy in range(NY)]
        out = []
        for yy in range(0, NY, 2):
            a, b = (jnp.concatenate([cand[2 * kind][t, mine], cand[2 * kind + 1][t, mine]], axis=1) for t in (yy, yy + 1))
            top = jnp.where(left16, a, swap(b))
            low = jnp.where(left16, swap(a), b)
            out.append(jnp.stack([top, low], axis=1).reshape(256, 128))
        return out

    def partial(q, kind):
        s2 = jnp.zeros((256, 128), F32)
        dd = jnp.zeros((256, 128), F32)
        g = jnp.zeros((256, 256), F32)
        xs = operands(q, kind)
        at = (0, 4, 6)[kind]
        for k in range(0, len(xs), 2):
            his, los = [], []
            for t in (k, k + 1):
                v = xs[t]
                s2 = s2 + v * v
                dd = dd + v * qrow[q, at + t:at + t + 1, :]
                hi = v.astype(jnp.bfloat16)
                his.append(hi)
                los.append((v - hi.astype(F32)).astype(jnp.bfloat16))
            hi = jnp.concatenate(his, axis=1)
            lo = jnp.concatenate(los, axis=1)
            g = g + (nt(hi, hi) + (nt(hi, lo) + nt(lo, hi)))
        return g, s2, dd

    def query_rows():
        row16 = lax.broadcasted_iota(jnp.int32, (16, 256), 0)
        left = lax.broadcasted_iota(jnp.int32, (1, 128), 1) < 64
        for q in range(4):
            rows = [jnp.sum(jnp.where(row16 == 4 * y + q, qall[yy], 0.0), axis=0, keepdims=True) for yy in range(NY)]
            for yy in range(NY):
                qrow[q, yy:yy + 1, :] = rows[yy][:, 0:128]
            far = [v[:, 128:256] for v in rows]
            for k in range(2):
                qrow[q, 4 + k:5 + k, :] = jnp.where(left, far[2 * k], swap(far[2 * k + 1]))
                qrow[q, 6 + k:7 + k, :] = jnp.where(left, swap(far[2 * k]), far[2 * k + 1])

    hop1, hop2, hop3 = {}, {}, {}
    for stage, ch, *more in STEPS:
        if stage == 1:
            hop1[ch] = stage1(ch)
            if ch == 1:
                for cp in qcopies:
                    cp.wait_recv()
                query_rows()
        elif stage == 2:
            hop2[ch] = stage2(ch, hop1[ch])
        elif stage == 3:
            hop3[ch] = (across_last if ch == NCH - 1 else across)(ch, hop2[ch])
        elif stage == "wait":
            for cp in hop3[ch]:
                cp.wait_recv()
        else:
            q = more[0]
            g, s2, dd = partial(q, ch)
            acc[q] = g if ch == 0 else acc[q] + g
            sq[q] = s2 if ch == 0 else sq[q] + s2
            dt[q] = dd if ch == 0 else dt[q] + dd
    for cp in hop3[NCH - 2]:
        cp.wait_recv()

    lane = lax.broadcasted_iota(jnp.int32, (256, 128), 1)
    outs = []
    for q in range(4):
        for cp in hop3[NCH - 1][3 * q:3 * q + 3]:
            cp.wait_recv()
        g, s2, dd = partial(q, 2)
        g = g + acc[q]
        rn = 1.0 / jnp.sqrt(jnp.sum(s2 + sq[q], axis=1, keepdims=True) + EPS)
        dots = jnp.sum(dd + dt[q], axis=1, keepdims=True)
        qv = qrow[q]
        qn = jnp.sqrt(jnp.sum(jnp.sum(qv * qv, axis=0, keepdims=True), axis=1, keepdims=True) + EPS)
        score = (scale * dots) * (rn / qn)
        flat = jnp.where(lane == 0, score, rn).T
        gsend[q] = g * flat[1:2, :]
        ssend[q] = flat[0:2, :]
        for d in (1, 3, 2):
            y2 = up(y, d, NY)
            outs.append(remote(gsend.at[q, pl.ds(y2 * 64, 64)], part_out.at[y * 4 + q], gs.at[q, d - 1], gr.at[q, d - 1], dev(y2, z, x, c)))
            outs.append(remote(ssend.at[q], vec_out.at[y * 4 + q], ss.at[q, d - 1], sr.at[q, d - 1], dev(y2, z, x, c)))
        part_out[y * 4 + q] = gsend[q, pl.ds(pl.multiple_of(y * 64, 64), 64)]
        vec_out[y * 4 + q] = ssend[q]
    for cp in outs:
        cp.wait_recv()
    for cp in sends:
        cp.wait_send()


def main_call(scale, ids, query, slab):
    dma = pltpu.SemaphoreType.DMA
    vm = pltpu.VMEM
    vmem = pl.BlockSpec(memory_space=pltpu.VMEM)
    anywhere = pl.BlockSpec(memory_space=pl.ANY)
    sizes = [n for n, _, _ in CHUNKS]
    return pl.pallas_call(
        functools.partial(main_kernel, scale),
        out_shape=(pltpu.VMEM((16, 64, 256), F32), pltpu.VMEM((16, 2, 256), F32)),
        in_specs=[anywhere, anywhere, anywhere],
        out_specs=(vmem, vmem),
        scratch_shapes=[
            vm(slab.shape, F32), vm((16, 16), jnp.int32), vm((NY, 16, 256), F32), vm((4, 8, 128), F32),
            vm((4, 1, 128), jnp.int32), vm((4, 1, 128), jnp.int32), vm((8, 4, 1, 128), jnp.int32),
            pltpu.SMEM((8, 4, 1, 128), jnp.int32), vm((2, 1, 128), jnp.int32), pltpu.SMEM((2, 1, 128), jnp.int32),
            *[vm((4, 8, HALF, n, 128), F32) for _ in range(4) for n in sizes],
            *[vm((NZ, NC, NX, CAP, n, 128), F32) for n in sizes],
            *[vm((3, 64, n, 128), F32) for n in sizes],
            *[vm((NY, 64, n, 128), F32) for n in sizes],
            vm((4, 256, 256), F32), vm((4, 256, 128), F32), vm((4, 256, 128), F32),
            vm((4, 256, 256), F32), vm((4, 2, 256), F32),
            dma(()), dma(()), dma(()), dma(()), dma(()), dma((3,)), dma((3,)), dma((7,)), dma((7,)),
            dma((NCH, 2, 3)), dma((NCH, 2, 3)), dma((NCH, 2, 7)), dma((NCH, 2, 7)),
            dma((NCH, 3)), dma((NCH, 3)), dma((4, 3)), dma((4, 3)), dma((3,)), dma((3,)),
            dma((4, 3)), dma((4, 3)), dma((4, 3)), dma((4, 3)),
        ],
        compiler_params=pltpu.CompilerParams(collective_id=0, has_side_effects=True, vmem_limit_bytes=58 * 2**20),
    )(ids, query, slab)


def per_device(slab, queries, block_ids):
    query_count, width_part = queries.shape
    full_width = width_part * lax.axis_size("pb")
    blocks_each = slab.shape[0] // BLOCK
    part, vec = main_call(math.sqrt(full_width), block_ids, queries, slab.reshape(blocks_each, BLOCK, width_part))
    own = lax.dynamic_slice_in_dim(vec, lax.axis_index("pb") * 64, 64, 2)
    scores = vec[:, 0]
    gram = part * own[:, 1][:, :, None]
    penalty = gram * jax.nn.sigmoid(scores[:, None, :] - own[:, 0][:, :, None])
    return (scores, gram, penalty)


def solution(mesh):
    return jax.shard_map(
        per_device,
        mesh=mesh,
        in_specs=(P("db", "pb"), P("db", "pb"), P("db", None)),
        out_specs=(P("db", None), P("db", "pb", None), P("db", "pb", None)),
        check_vma=False,
    )
```

```python
import functools
import math

import jax
import jax.numpy as jnp
from jax import lax
from jax.experimental import pallas as pl
from jax.experimental.pallas import tpu as pltpu
from jax.sharding import PartitionSpec as P

BLOCK = 16
CAP = 12
HALF = 6
NZ, NX, NC, NY = 4, 4, 2, 4
EPS = 1e-06
MESH = pl.DeviceIdType.MESH
F32 = jnp.float32
CHUNKS = ((8, 0, 0), (8, 8, 0), (4, 0, 1), (4, 4, 1), (4, 0, 2), (2, 4, 2), (2, 6, 2))
NCH = len(CHUNKS)
STEPS = ((1, 0), (1, 1), (2, 0), (1, 2), (2, 1), (1, 3), (3, 0), (2, 2), (1, 4), (3, 1), (2, 3), (1, 5), (3, 2), ("wait", 0), ("wait", 1),
         ("sum", 0, 0), ("sum", 0, 1), (2, 4), (1, 6), ("sum", 0, 2), ("sum", 0, 3), (3, 3), (2, 5), (3, 4), (2, 6), ("wait", 2), ("wait", 3),
         ("sum", 1, 0), ("sum", 1, 1), ("sum", 1, 2), ("sum", 1, 3), (3, 5), (3, 6))
WIDE = [(d, e) for d in range(4) for e in range(2) if (d, e) != (0, 0)]


def main_kernel(scale, ids, query, slab, part_out, vec_out, slabv, idv, qall, qrow, tab, tmid, tfin, tsm, pos, psm, *rest):
    src_a, mid_a, src_b, mid_b, fin, ysend, cand = (rest[i * NCH:(i + 1) * NCH] for i in range(7))
    (acc, sq, dt, gsend, ssend,
     lsem, isem, psem, tsem, qsem, ts1, tr1, ts2, tr2, qs, qr, s1s, s1r, s2s, s2r, ys, yr, zr, gs, gr, ss, sr) = rest[7 * NCH:]
    y = lax.axis_index("pb")
    db = lax.axis_index("db")
    z, x, c = db // (NX * NC), (db // NC) % NX, db % NC
    jx = x * NC + c
    jz = z * NC + c

    def dev(yy, zz, xx, cc):
        return (yy, (zz * NX + xx) * NC + cc)

    def up(v, d, n):
        return (v + d) % n

    peers = [dev(y, up(z, d, NZ), x, up(c, e, NC)) for d, e in WIDE]
    peers += [dev(y, z, up(x, d, NX), up(c, e, NC)) for d, e in WIDE if d]
    peers += [dev(up(y, d, NY), z, x, c) for d in range(1, NY)]
    barrier = pltpu.get_barrier_semaphore()
    for p in peers:
        pl.semaphore_signal(barrier, inc=1, device_id=p, device_id_type=MESH)
    icopy = pltpu.make_async_copy(ids, idv, isem)
    icopy.start()
    qcopy = pltpu.make_async_copy(query, qall.at[y], qsem)
    qcopy.start()
    load = pltpu.make_async_copy(slab, slabv, lsem)
    load.start()

    icopy.wait()
    wide = jnp.concatenate([idv[...]] * 8, axis=1)
    sub = lax.broadcasted_iota(jnp.int32, (16, 128), 0)
    lan = lax.broadcasted_iota(jnp.int32, (16, 128), 1)
    wide = jnp.where(lan // 16 == sub % 8, wide, 0)
    row = [jnp.sum(wide[8 * i:8 * i + 8], axis=0, keepdims=True) for i in range(2)]
    big_r = lax.broadcasted_iota(jnp.int32, (128, 128), 0)
    big_c = lax.broadcasted_iota(jnp.int32, (128, 128), 1)

    def column(v):
        return jnp.broadcast_to(v, (128, 128)).T

    each = slab.shape[0]
    own = [v // each for v in row]
    own_t = [column(v) for v in own]
    rank = [jnp.sum(jnp.where((own_t[0] == own[0]) & (big_r < big_c), 1, 0), axis=0, keepdims=True),
            jnp.sum(jnp.where(own_t[0] == own[1], 1, 0), axis=0, keepdims=True)
            + jnp.sum(jnp.where((own_t[1] == own[1]) & (big_r < big_c), 1, 0), axis=0, keepdims=True)]
    code_t = [column((own[i] * 16 + rank[i]) * each + row[i] % each) for i in range(2)]
    for zz in range(NZ):
        tab[zz] = sum(jnp.sum(jnp.where(code_t[i] // each == big_c + 128 * zz, code_t[i] % each, 0), axis=0, keepdims=True)
                      for i in range(2))
    for i in range(2):
        o = own[i]
        pos[i] = (((o // 8) * NC + o % 2) * NX + (o // 2) % 4) * CAP + rank[i]
    pcopy = pltpu.make_async_copy(pos, psm, psem)
    pcopy.start()
    tmid[z] = tab[z]

    pl.semaphore_wait(barrier, len(peers))

    def copy(src, dst, ssem, rsem, target):
        return pltpu.make_async_remote_copy(src_ref=src, dst_ref=dst, send_sem=ssem, recv_sem=rsem,
                                            device_id=target, device_id_type=MESH)

    def remote(*args):
        copy(*args).start()

    def arrived(view, sem):
        copy(view, view, sem, sem, peers[0]).wait_recv()

    def left(view, sem):
        copy(view, view, sem, sem, peers[0]).wait_send()

    for d in range(1, NZ):
        remote(tab.at[up(z, d, NZ)], tmid.at[z], ts1, tr1, dev(y, up(z, d, NZ), x, c))
    qcopy.wait()
    for d in range(1, NY):
        remote(qall.at[y], qall.at[y], qs, qr, dev(up(y, d, NY), z, x, c))
    arrived(tmid.at[0:3], tr1)
    for d, e in WIDE:
        remote(tmid, tfin.at[jx], ts2, tr2, dev(y, z, up(x, d, NX), up(c, e, NC)))
    tfin[jx] = tmid[...]
    arrived(tfin.at[0:7], tr2)
    tcopy = pltpu.make_async_copy(tfin, tsm, tsem)
    tcopy.start()
    load.wait()
    pcopy.wait()
    tcopy.wait()

    def tile(ch, at):
        n, r0, kind = CHUNKS[ch]
        if kind == 0:
            return slabv[at, r0:r0 + n, 0:128]
        top = slabv[at, r0:r0 + n, 128:256]
        low = slabv[at, 8 + r0:8 + r0 + n, 128:256]
        left = lax.broadcasted_iota(jnp.int32, (n, 128), 1) < 64
        if kind == 1:
            return jnp.where(left, top, pltpu.roll(low, 64, 1))
        return jnp.where(left, pltpu.roll(top, 64, 1), low)

    def gather(ch):
        for d in range(4):
            z2, x2 = up(z, d, NZ), up(x, d, NX)
            to_a = mid_a[ch] if d == 0 else src_a[ch]
            to_b = mid_b[ch] if d == 0 else src_b[ch]

            def body(j, carry):
                for s in range(HALF):
                    to_a[z2, j, s] = tile(ch, tsm[j, z2, 0, jx * 16 + s])
                for s in range(HALF):
                    to_b[x2, j, s] = tile(ch, tsm[x2 * NC + j % NC, j // NC, 0, jx * 16 + HALF + s])
                return carry

            lax.fori_loop(0, 8, body, 0)

    def stage1(ch):
        gather(ch)
        for d in (1, 3, 2):
            z2, x2 = up(z, d, NZ), up(x, d, NX)
            remote(src_a[ch].at[z2], mid_a[ch].at[z], s1s, s1r.at[ch, 0], dev(y, z2, x, c))
            remote(src_b[ch].at[x2], mid_b[ch].at[x], s1s, s1r.at[ch, 1], dev(y, z, x2, c))

    def stage2(ch):
        arrived(mid_a[ch].at[0:3], s1r.at[ch, 0])
        arrived(mid_b[ch].at[0:3], s1r.at[ch, 1])
        for d, e in WIDE:
            z2, x2, c2 = up(z, d, NZ), up(x, d, NX), up(c, e, NC)
            remote(mid_a[ch].at[:, x2 * NC + c2], fin[ch].at[:, c, x, 0:HALF], s2s, s2r.at[ch, 0], dev(y, z, x2, c2))
            remote(mid_b[ch].at[:, z2 * NC + c2], fin[ch].at[z, c, :, HALF:CAP], s2s, s2r.at[ch, 1], dev(y, z2, x, c2))
        for i in range(4):
            fin[ch][i, c, x, 0:HALF] = mid_a[ch][i, jx]
            fin[ch][z, c, i, HALF:CAP] = mid_b[ch][i, jz]

    def both_arrived(ch):
        arrived(mid_a[ch].at[:, 0:7], s2r.at[ch, 0])
        arrived(mid_b[ch].at[:, 0:7], s2r.at[ch, 1])

    def pick(ch, y2, q, out):
        flat = fin[ch].reshape(NZ * NC * NX * CAP, CHUNKS[ch][0], 128)
        upper = y2 // 2
        base = (y2 % 2) * 64 + q * 16
        for u in range(16):
            out[q * 16 + u] = flat[psm[upper, 0, base + u]]

    def across(ch):
        both_arrived(ch)
        for d in (1, 3, 2, 0):
            y2 = up(y, d, NY)
            out = ysend[ch].at[d - 1] if d else cand[ch].at[y]

            def body(q, carry):
                pick(ch, y2, q, out)
                return carry

            lax.fori_loop(0, 4, body, 0)
            if d:
                remote(out, cand[ch].at[y], ys, yr.at[ch], dev(y2, z, x, c))

    def across_last(ch):
        both_arrived(ch)
        for q in range(4):
            mine = pl.ds(q * 16, 16)
            for d in (1, 3, 2, 0):
                y2 = up(y, d, NY)
                out = ysend[ch].at[d - 1] if d else cand[ch].at[y]
                pick(ch, y2, q, out)
                if d:
                    remote(out.at[mine], cand[ch].at[y, mine], ys, zr.at[q], dev(y2, z, x, c))

    def nt(a, b):
        return lax.dot_general(a, b, (((1,), (1,)), ((), ())), preferred_element_type=F32)

    left16 = lax.broadcasted_iota(jnp.int32, (16, 8, 128), 2) < 64

    def swap(v):
        return pltpu.roll(v, 64, v.ndim - 1)

    def operands(q, kind):
        mine = pl.ds(q * 16, 16)
        if kind == 0:
            return [jnp.stack([cand[0][yy, mine], cand[1][yy, mine]], axis=1).reshape(256, 128) for yy in range(NY)]
        out = []
        for yy in range(0, NY, 2):
            a, b = (jnp.concatenate([cand[ch][t, mine] for ch in range(NCH) if CHUNKS[ch][2] == kind], axis=1) for t in (yy, yy + 1))
            top = jnp.where(left16, a, swap(b))
            low = jnp.where(left16, swap(a), b)
            out.append(jnp.stack([top, low], axis=1).reshape(256, 128))
        return out

    def partial(q, kind):
        s2 = jnp.zeros((256, 128), F32)
        dd = jnp.zeros((256, 128), F32)
        g = jnp.zeros((256, 256), F32)
        xs = operands(q, kind)
        at = (0, 4, 6)[kind]
        for k in range(0, len(xs), 2):
            his, los = [], []
            for t in (k, k + 1):
                v = xs[t]
                s2 = s2 + v * v
                dd = dd + v * qrow[q, at + t:at + t + 1, :]
                hi = v.astype(jnp.bfloat16)
                his.append(hi)
                los.append((v - hi.astype(F32)).astype(jnp.bfloat16))
            hi = jnp.concatenate(his, axis=1)
            lo = jnp.concatenate(los, axis=1)
            g = g + (nt(hi, hi) + (nt(hi, lo) + nt(lo, hi)))
        return g, s2, dd

    def query_rows():
        row16 = lax.broadcasted_iota(jnp.int32, (16, 256), 0)
        left = lax.broadcasted_iota(jnp.int32, (1, 128), 1) < 64
        for q in range(4):
            rows = [jnp.sum(jnp.where(row16 == 4 * y + q, qall[yy], 0.0), axis=0, keepdims=True) for yy in range(NY)]
            for yy in range(NY):
                qrow[q, yy:yy + 1, :] = rows[yy][:, 0:128]
            far = [v[:, 128:256] for v in rows]
            for k in range(2):
                qrow[q, 4 + k:5 + k, :] = jnp.where(left, far[2 * k], swap(far[2 * k + 1]))
                qrow[q, 6 + k:7 + k, :] = jnp.where(left, swap(far[2 * k]), far[2 * k + 1])

    for stage, ch, *more in STEPS:
        if stage == 1:
            stage1(ch)
            if ch == 1:
                arrived(qall.at[0:3], qr)
                query_rows()
        elif stage == 2:
            stage2(ch)
        elif stage == 3:
            (across_last if ch == NCH - 1 else across)(ch)
        elif stage == "wait":
            arrived(cand[ch].at[0:3], yr.at[ch])
        else:
            q = more[0]
            g, s2, dd = partial(q, ch)
            acc[q] = g if ch == 0 else acc[q] + g
            sq[q] = s2 if ch == 0 else sq[q] + s2
            dt[q] = dd if ch == 0 else dt[q] + dd
    for ch in range(NCH - 1):
        if CHUNKS[ch][2] == 2:
            arrived(cand[ch].at[0:3], yr.at[ch])

    lane = lax.broadcasted_iota(jnp.int32, (256, 128), 1)
    for q in range(4):
        arrived(cand[NCH - 1].at[0:3, pl.ds(q * 16, 16)], zr.at[q])
        g, s2, dd = partial(q, 2)
        g = g + acc[q]
        rn = 1.0 / jnp.sqrt(jnp.sum(s2 + sq[q], axis=1, keepdims=True) + EPS)
        dots = jnp.sum(dd + dt[q], axis=1, keepdims=True)
        qv = qrow[q]
        qn = jnp.sqrt(jnp.sum(jnp.sum(qv * qv, axis=0, keepdims=True), axis=1, keepdims=True) + EPS)
        score = (scale * dots) * (rn / qn)
        flat = jnp.where(lane == 0, score, rn).T
        gsend[q] = g * flat[1:2, :]
        ssend[q] = flat[0:2, :]
        for d in (1, 3, 2):
            y2 = up(y, d, NY)
            remote(gsend.at[q, pl.ds(y2 * 64, 64)], part_out.at[y * 4 + q], gs, gr, dev(y2, z, x, c))
            remote(ssend.at[q], vec_out.at[y * 4 + q], ss, sr, dev(y2, z, x, c))
        part_out[y * 4 + q] = gsend[q, pl.ds(pl.multiple_of(y * 64, 64), 64)]
        vec_out[y * 4 + q] = ssend[q]
    arrived(part_out.at[0:12], gr)
    arrived(vec_out.at[0:12], sr)
    left(part_out.at[0:12], gs)
    left(vec_out.at[0:12], ss)
    left(tmid.at[0:3], ts1)
    left(tfin.at[0:7], ts2)
    left(qall.at[0:3], qs)
    left(slabv.at[0:288], s1s)
    left(slabv.at[0:336], s2s)
    left(slabv.at[0:192], ys)


def main_call(scale, ids, query, slab):
    dma = pltpu.SemaphoreType.DMA
    vm = pltpu.VMEM
    vmem = pl.BlockSpec(memory_space=pltpu.VMEM)
    anywhere = pl.BlockSpec(memory_space=pl.ANY)
    sizes = [n for n, _, _ in CHUNKS]
    return pl.pallas_call(
        functools.partial(main_kernel, scale),
        out_shape=(pltpu.VMEM((16, 64, 256), F32), pltpu.VMEM((16, 2, 256), F32)),
        in_specs=[anywhere, anywhere, anywhere],
        out_specs=(vmem, vmem),
        scratch_shapes=[
            vm(slab.shape, F32), vm((16, 16), jnp.int32), vm((NY, 16, 256), F32), vm((4, 8, 128), F32),
            vm((4, 1, 128), jnp.int32), vm((4, 1, 128), jnp.int32), vm((8, 4, 1, 128), jnp.int32),
            pltpu.SMEM((8, 4, 1, 128), jnp.int32), vm((2, 1, 128), jnp.int32), pltpu.SMEM((2, 1, 128), jnp.int32),
            *[vm((4, 8, HALF, n, 128), F32) for _ in range(4) for n in sizes],
            *[vm((NZ, NC, NX, CAP, n, 128), F32) for n in sizes],
            *[vm((3, 64, n, 128), F32) for n in sizes],
            *[vm((NY, 64, n, 128), F32) for n in sizes],
            vm((4, 256, 256), F32), vm((4, 256, 128), F32), vm((4, 256, 128), F32),
            vm((4, 256, 256), F32), vm((4, 2, 256), F32),
            *[dma(()) for _ in range(12)], dma((NCH, 2)), dma(()), dma((NCH, 2)), dma(()), dma((NCH,)), dma((4,)), *[dma(()) for _ in range(4)],
        ],
        compiler_params=pltpu.CompilerParams(collective_id=0, has_side_effects=True, vmem_limit_bytes=58 * 2**20),
    )(ids, query, slab)


def per_device(slab, queries, block_ids):
    query_count, width_part = queries.shape
    full_width = width_part * lax.axis_size("pb")
    blocks_each = slab.shape[0] // BLOCK
    part, vec = main_call(math.sqrt(full_width), block_ids, queries, slab.reshape(blocks_each, BLOCK, width_part))
    own = lax.dynamic_slice_in_dim(vec, lax.axis_index("pb") * 64, 64, 2)
    scores = vec[:, 0]
    gram = part * own[:, 1][:, :, None]
    penalty = gram * jax.nn.sigmoid(scores[:, None, :] - own[:, 0][:, :, None])
    return (scores, gram, penalty)


def solution(mesh):
    return jax.shard_map(
        per_device,
        mesh=mesh,
        in_specs=(P("db", "pb"), P("db", "pb"), P("db", None)),
        out_specs=(P("db", None), P("db", "pb", None), P("db", "pb", None)),
        check_vma=False,
    )
```

```python
import functools
import math

import jax
import jax.numpy as jnp
from jax import lax
from jax.experimental import pallas as pl
from jax.experimental.pallas import tpu as pltpu
from jax.sharding import PartitionSpec as P

BLOCK = 16
CAP = 12
HALF = 6
NZ, NX, NC, NY = 4, 4, 2, 4
EPS = 1e-06
MESH = pl.DeviceIdType.MESH
F32 = jnp.float32
CHUNKS = ((8, 0, 0), (8, 8, 0), (4, 0, 1), (4, 4, 1), (2, 0, 2), (2, 2, 2), (2, 4, 2), (2, 6, 2))
NCH = len(CHUNKS)
STEPS = ((1, 1), (2, 0), (1, 2), (2, 1), (1, 3), (3, 0), (2, 2), (1, 4), (3, 1), (2, 3), (1, 5), ("wait", 0), (3, 2), ("wait", 1),
         ("sum", 0, 0), ("sum", 0, 1), (2, 4), (1, 6), ("sum", 0, 2), (3, 3), ("sum", 0, 3), (2, 5), (1, 7), (3, 4), (2, 6), (3, 5), (2, 7),
         ("wait", 2), ("wait", 3), ("sum", 1, 0), ("sum", 1, 1), ("sum", 1, 2), ("sum", 1, 3), (3, 6), (3, 7))
WIDE = [(d, e) for d in range(4) for e in range(2) if (d, e) != (0, 0)]


def main_kernel(scale, ids, query, slab, part_out, vec_out, slabv, idv, qall, qrow, tab, near, far, nsm, fsm, pos, psm, *rest):
    src_a, mid_a, src_b, mid_b, fin, ysend, cand = (rest[i * NCH:(i + 1) * NCH] for i in range(7))
    (acc, sq, dt, gsend, ssend,
     lsem, isem, psem, nsem, fsem, qsem, ts1, tr1, ts2, tr2, qs, qr, s1s, s1r, s2s, s2r, ys, yr, zr, gs, gr, ss, sr) = rest[7 * NCH:]
    y = lax.axis_index("pb")
    db = lax.axis_index("db")
    z, x, c = db // (NX * NC), (db // NC) % NX, db % NC
    jx = x * NC + c
    jz = z * NC + c

    def dev(yy, zz, xx, cc):
        return (yy, (zz * NX + xx) * NC + cc)

    def up(v, d, n):
        return (v + d) % n

    peers = [dev(y, up(z, d, NZ), x, up(c, e, NC)) for d, e in WIDE]
    peers += [dev(y, z, up(x, d, NX), up(c, e, NC)) for d, e in WIDE if d]
    peers += [dev(up(y, d, NY), z, x, c) for d in range(1, NY)]
    barrier = pltpu.get_barrier_semaphore()
    for p in peers:
        pl.semaphore_signal(barrier, inc=1, device_id=p, device_id_type=MESH)
    icopy = pltpu.make_async_copy(ids, idv, isem)
    icopy.start()
    qcopy = pltpu.make_async_copy(query, qall.at[y], qsem)
    qcopy.start()
    load = pltpu.make_async_copy(slab, slabv, lsem)
    load.start()

    icopy.wait()
    wide = jnp.concatenate([idv[...]] * 8, axis=1)
    sub = lax.broadcasted_iota(jnp.int32, (16, 128), 0)
    lan = lax.broadcasted_iota(jnp.int32, (16, 128), 1)
    wide = jnp.where(lan // 16 == sub % 8, wide, 0)
    row = [jnp.sum(wide[8 * i:8 * i + 8], axis=0, keepdims=True) for i in range(2)]
    big_r = lax.broadcasted_iota(jnp.int32, (128, 128), 0)
    big_c = lax.broadcasted_iota(jnp.int32, (128, 128), 1)

    def column(v):
        return jnp.broadcast_to(v, (128, 128)).T

    each = slab.shape[0]
    own = [v // each for v in row]
    own_t = [column(v) for v in own]
    rank = [jnp.sum(jnp.where((own_t[0] == own[0]) & (big_r < big_c), 1, 0), axis=0, keepdims=True),
            jnp.sum(jnp.where(own_t[0] == own[1], 1, 0), axis=0, keepdims=True)
            + jnp.sum(jnp.where((own_t[1] == own[1]) & (big_r < big_c), 1, 0), axis=0, keepdims=True)]
    code_t = [column((own[i] * 16 + rank[i]) * each + row[i] % each) for i in range(2)]
    for zz in range(NZ):
        tab[zz] = sum(jnp.sum(jnp.where(code_t[i] // each == big_c + 128 * zz, code_t[i] % each, 0), axis=0, keepdims=True)
                      for i in range(2))
    for i in range(2):
        o = own[i]
        pos[i] = (((o // 8) * NC + o % 2) * NX + (o // 2) % 4) * CAP + rank[i]
    pcopy = pltpu.make_async_copy(pos, psm, psem)
    pcopy.start()
    near[z * NC + c] = tab[z]
    near[8 + jx] = tab[z]
    near[8 + x * NC + 1 - c] = tab[z]

    pl.semaphore_wait(barrier, len(peers))

    def copy(src, dst, ssem, rsem, target):
        return pltpu.make_async_remote_copy(src_ref=src, dst_ref=dst, send_sem=ssem, recv_sem=rsem,
                                            device_id=target, device_id_type=MESH)

    def remote(*args):
        copy(*args).start()

    def arrived(view, sem):
        copy(view, view, sem, sem, peers[0]).wait_recv()

    def left(view, sem):
        copy(view, view, sem, sem, peers[0]).wait_send()

    for d, e in WIDE:
        z2, c2 = up(z, d, NZ), up(c, e, NC)
        remote(tab.at[z2], near.at[z * NC + c], ts1, tr1, dev(y, z2, x, c2))
        if d:
            x2 = up(x, d, NX)
            remote(tab.at[z], near.at[8 + jx], ts1, tr1, dev(y, z, x2, c2))
    arrived(near.at[0:13], tr1)
    ncopy = pltpu.make_async_copy(near, nsm, nsem)
    ncopy.start()
    for d in range(1, NX):
        remote(near.at[0:8], far.at[x], ts2, tr2, dev(y, z, up(x, d, NX), c))
    far[x] = near[0:8]
    load.wait()
    ncopy.wait()

    def tile(ch, at):
        n, r0, kind = CHUNKS[ch]
        if kind == 0:
            return slabv[at, r0:r0 + n, 0:128]
        top = slabv[at, r0:r0 + n, 128:256]
        low = slabv[at, 8 + r0:8 + r0 + n, 128:256]
        left = lax.broadcasted_iota(jnp.int32, (n, 128), 1) < 64
        if kind == 1:
            return jnp.where(left, top, pltpu.roll(low, 64, 1))
        return jnp.where(left, pltpu.roll(top, 64, 1), low)

    def fill(ch, to, at, row, first):
        for s in range(HALF):
            to[ch][(*at, s)] = tile(ch, row(jx * 16 + first + s))

    def gather(ch):
        for d in range(4):
            z2, x2 = up(z, d, NZ), up(x, d, NX)

            def body(j, carry):
                fill(ch, src_a if d else mid_a, (z2, j), lambda k: fsm[j // NC, z2 * NC + j % NC, 0, k], 0)
                fill(ch, src_b if d else mid_b, (x2, j), lambda k: fsm[x2, j, 0, k], HALF)
                return carry

            lax.fori_loop(0, 8, body, 0)

    def open_near():
        for d in range(4):
            z2, x2 = up(z, d, NZ), up(x, d, NX)
            line = (8 + x2 * NC) if d else z * NC

            def body(e, carry):
                if d:
                    fill(0, src_a, (z2, x * NC + e), lambda k: nsm[z2 * NC + e, 0, k], 0)
                    fill(0, src_b, (x2, z * NC + e), lambda k: nsm[line + e, 0, k], HALF)
                fill(0, mid_a, (z, x2 * NC + e), lambda k: nsm[line + e, 0, k], 0)
                fill(0, mid_b, (x, z2 * NC + e), lambda k: nsm[z2 * NC + e, 0, k], HALF)
                return carry

            lax.fori_loop(0, 2, body, 0)
        for d in (1, 3, 2):
            z2, x2 = up(z, d, NZ), up(x, d, NX)
            mine_a, mine_b = pl.ds(x * NC, NC), pl.ds(z * NC, NC)
            remote(src_a[0].at[z2, mine_a], mid_a[0].at[z, mine_a], s1s, s1r.at[0, 0], dev(y, z2, x, c))
            remote(src_b[0].at[x2, mine_b], mid_b[0].at[x, mine_b], s1s, s1r.at[0, 1], dev(y, z, x2, c))
        for d, e in WIDE:
            z2, x2, c2 = up(z, d, NZ), up(x, d, NX), up(c, e, NC)
            remote(mid_a[0].at[z, x2 * NC + c2], fin[0].at[z, c, x, 0:HALF], s2s, s2r.at[0, 0], dev(y, z, x2, c2))
            remote(mid_b[0].at[x, z2 * NC + c2], fin[0].at[z, c, x, HALF:CAP], s2s, s2r.at[0, 1], dev(y, z2, x, c2))

    def open_far():
        for d in range(1, 4):
            z2, x2 = up(z, d, NZ), up(x, d, NX)

            def body(i, carry):
                k2, e = up(i // NC, 1, 4), i % NC
                z3, x3 = up(z, k2, NZ), up(x, k2, NX)
                fill(0, src_a, (z2, x3 * NC + e), lambda k: fsm[x3, z2 * NC + e, 0, k], 0)
                fill(0, src_b, (x2, z3 * NC + e), lambda k: fsm[x2, z3 * NC + e, 0, k], HALF)
                return carry

            lax.fori_loop(0, 6, body, 0)
        for d in (1, 3, 2):
            for k2 in range(1, 4):
                z2, x2 = up(z, d, NZ), up(x, d, NX)
                their_a, their_b = pl.ds(up(x, k2, NX) * NC, NC), pl.ds(up(z, k2, NZ) * NC, NC)
                remote(src_a[0].at[z2, their_a], mid_a[0].at[z, their_a], s1s, s1r.at[0, 0], dev(y, z2, x, c))
                remote(src_b[0].at[x2, their_b], mid_b[0].at[x, their_b], s1s, s1r.at[0, 1], dev(y, z, x2, c))

    def stage1(ch):
        gather(ch)
        for d in (1, 3, 2):
            z2, x2 = up(z, d, NZ), up(x, d, NX)
            remote(src_a[ch].at[z2], mid_a[ch].at[z], s1s, s1r.at[ch, 0], dev(y, z2, x, c))
            remote(src_b[ch].at[x2], mid_b[ch].at[x], s1s, s1r.at[ch, 1], dev(y, z, x2, c))

    def stage2(ch):
        arrived(mid_a[ch].at[0:3], s1r.at[ch, 0])
        arrived(mid_b[ch].at[0:3], s1r.at[ch, 1])
        for d, e in WIDE:
            z2, x2, c2 = up(z, d, NZ), up(x, d, NX), up(c, e, NC)
            if ch:
                remote(mid_a[ch].at[:, x2 * NC + c2], fin[ch].at[:, c, x, 0:HALF], s2s, s2r.at[ch, 0], dev(y, z, x2, c2))
                remote(mid_b[ch].at[:, z2 * NC + c2], fin[ch].at[z, c, :, HALF:CAP], s2s, s2r.at[ch, 1], dev(y, z2, x, c2))
            else:
                for k2 in range(1, 4):
                    z3, x3 = up(z, k2, NZ), up(x, k2, NX)
                    remote(mid_a[0].at[z3, x2 * NC + c2], fin[0].at[z3, c, x, 0:HALF], s2s, s2r.at[0, 0], dev(y, z, x2, c2))
                    remote(mid_b[0].at[x3, z2 * NC + c2], fin[0].at[z, c, x3, HALF:CAP], s2s, s2r.at[0, 1], dev(y, z2, x, c2))
        for i in range(4):
            fin[ch][i, c, x, 0:HALF] = mid_a[ch][i, jx]
            fin[ch][z, c, i, HALF:CAP] = mid_b[ch][i, jz]

    def both_arrived(ch):
        arrived(mid_a[ch].at[:, 0:7], s2r.at[ch, 0])
        arrived(mid_b[ch].at[:, 0:7], s2r.at[ch, 1])

    def pick(ch, y2, q, out):
        flat = fin[ch].reshape(NZ * NC * NX * CAP, CHUNKS[ch][0], 128)
        upper = y2 // 2
        base = (y2 % 2) * 64 + q * 16
        for u in range(16):
            out[q * 16 + u] = flat[psm[upper, 0, base + u]]

    def across(ch):
        both_arrived(ch)
        for d in (1, 3, 2, 0):
            y2 = up(y, d, NY)
            out = ysend[ch].at[d - 1] if d else cand[ch].at[y]

            def body(q, carry):
                pick(ch, y2, q, out)
                return carry

            lax.fori_loop(0, 4, body, 0)
            if d:
                remote(out, cand[ch].at[y], ys, yr.at[ch], dev(y2, z, x, c))

    def across_last(ch):
        both_arrived(ch)
        for q in range(4):
            mine = pl.ds(q * 16, 16)
            for d in (1, 3, 2, 0):
                y2 = up(y, d, NY)
                out = ysend[ch].at[d - 1] if d else cand[ch].at[y]
                pick(ch, y2, q, out)
                if d:
                    remote(out.at[mine], cand[ch].at[y, mine], ys, zr.at[q], dev(y2, z, x, c))

    def nt(a, b):
        return lax.dot_general(a, b, (((1,), (1,)), ((), ())), preferred_element_type=F32)

    left16 = lax.broadcasted_iota(jnp.int32, (16, 8, 128), 2) < 64

    def swap(v):
        return pltpu.roll(v, 64, v.ndim - 1)

    def operands(q, kind):
        mine = pl.ds(q * 16, 16)
        if kind == 0:
            return [jnp.stack([cand[0][yy, mine], cand[1][yy, mine]], axis=1).reshape(256, 128) for yy in range(NY)]
        out = []
        for yy in range(0, NY, 2):
            a, b = (jnp.concatenate([cand[ch][t, mine] for ch in range(NCH) if CHUNKS[ch][2] == kind], axis=1) for t in (yy, yy + 1))
            top = jnp.where(left16, a, swap(b))
            low = jnp.where(left16, swap(a), b)
            out.append(jnp.stack([top, low], axis=1).reshape(256, 128))
        return out

    def partial(q, kind):
        s2 = jnp.zeros((256, 128), F32)
        dd = jnp.zeros((256, 128), F32)
        g = jnp.zeros((256, 256), F32)
        xs = operands(q, kind)
        at = (0, 4, 6)[kind]
        for k in range(0, len(xs), 2):
            his, los = [], []
            for t in (k, k + 1):
                v = xs[t]
                s2 = s2 + v * v
                dd = dd + v * qrow[q, at + t:at + t + 1, :]
                hi = v.astype(jnp.bfloat16)
                his.append(hi)
                los.append((v - hi.astype(F32)).astype(jnp.bfloat16))
            hi = jnp.concatenate(his, axis=1)
            lo = jnp.concatenate(los, axis=1)
            g = g + (nt(hi, hi) + (nt(hi, lo) + nt(lo, hi)))
        return g, s2, dd

    def query_rows():
        row16 = lax.broadcasted_iota(jnp.int32, (16, 256), 0)
        left = lax.broadcasted_iota(jnp.int32, (1, 128), 1) < 64
        for q in range(4):
            rows = [jnp.sum(jnp.where(row16 == 4 * y + q, qall[yy], 0.0), axis=0, keepdims=True) for yy in range(NY)]
            for yy in range(NY):
                qrow[q, yy:yy + 1, :] = rows[yy][:, 0:128]
            far = [v[:, 128:256] for v in rows]
            for k in range(2):
                qrow[q, 4 + k:5 + k, :] = jnp.where(left, far[2 * k], swap(far[2 * k + 1]))
                qrow[q, 6 + k:7 + k, :] = jnp.where(left, swap(far[2 * k]), far[2 * k + 1])

    open_near()
    arrived(far.at[0:3], tr2)
    fcopy = pltpu.make_async_copy(far, fsm, fsem)
    fcopy.start()
    qcopy.wait()
    for d in range(1, NY):
        remote(qall.at[y], qall.at[y], qs, qr, dev(up(y, d, NY), z, x, c))
    fcopy.wait()
    open_far()
    pcopy.wait()
    for stage, ch, *more in STEPS:
        if stage == 1:
            stage1(ch)
            if ch == 1:
                arrived(qall.at[0:3], qr)
                query_rows()
        elif stage == 2:
            stage2(ch)
        elif stage == 3:
            (across_last if ch == NCH - 1 else across)(ch)
        elif stage == "wait":
            arrived(cand[ch].at[0:3], yr.at[ch])
        else:
            q = more[0]
            g, s2, dd = partial(q, ch)
            acc[q] = g if ch == 0 else acc[q] + g
            sq[q] = s2 if ch == 0 else sq[q] + s2
            dt[q] = dd if ch == 0 else dt[q] + dd
    for ch in range(NCH - 1):
        if CHUNKS[ch][2] == 2:
            arrived(cand[ch].at[0:3], yr.at[ch])

    lane = lax.broadcasted_iota(jnp.int32, (256, 128), 1)
    for q in range(4):
        arrived(cand[NCH - 1].at[0:3, pl.ds(q * 16, 16)], zr.at[q])
        g, s2, dd = partial(q, 2)
        g = g + acc[q]
        rn = 1.0 / jnp.sqrt(jnp.sum(s2 + sq[q], axis=1, keepdims=True) + EPS)
        dots = jnp.sum(dd + dt[q], axis=1, keepdims=True)
        qv = qrow[q]
        qn = jnp.sqrt(jnp.sum(jnp.sum(qv * qv, axis=0, keepdims=True), axis=1, keepdims=True) + EPS)
        score = (scale * dots) * (rn / qn)
        flat = jnp.where(lane == 0, score, rn).T
        gsend[q] = g * flat[1:2, :]
        ssend[q] = flat[0:2, :]
        for d in (1, 3, 2):
            y2 = up(y, d, NY)
            remote(gsend.at[q, pl.ds(y2 * 64, 64)], part_out.at[y * 4 + q], gs, gr, dev(y2, z, x, c))
            remote(ssend.at[q], vec_out.at[y * 4 + q], ss, sr, dev(y2, z, x, c))
        part_out[y * 4 + q] = gsend[q, pl.ds(pl.multiple_of(y * 64, 64), 64)]
        vec_out[y * 4 + q] = ssend[q]
    arrived(part_out.at[0:12], gr)
    arrived(vec_out.at[0:12], sr)
    left(part_out.at[0:12], gs)
    left(vec_out.at[0:12], ss)
    left(near.at[0:13], ts1)
    left(far.at[0:3], ts2)
    left(qall.at[0:3], qs)
    left(slabv.at[0:288], s1s)
    left(slabv.at[0:336], s2s)
    left(slabv.at[0:192], ys)


def main_call(scale, ids, query, slab):
    dma = pltpu.SemaphoreType.DMA
    vm = pltpu.VMEM
    vmem = pl.BlockSpec(memory_space=pltpu.VMEM)
    anywhere = pl.BlockSpec(memory_space=pl.ANY)
    sizes = [n for n, _, _ in CHUNKS]
    return pl.pallas_call(
        functools.partial(main_kernel, scale),
        out_shape=(pltpu.VMEM((16, 64, 256), F32), pltpu.VMEM((16, 2, 256), F32)),
        in_specs=[anywhere, anywhere, anywhere],
        out_specs=(vmem, vmem),
        scratch_shapes=[
            vm(slab.shape, F32), vm((16, 16), jnp.int32), vm((NY, 16, 256), F32), vm((4, 8, 128), F32),
            vm((4, 1, 128), jnp.int32), vm((16, 1, 128), jnp.int32), vm((4, 8, 1, 128), jnp.int32),
            pltpu.SMEM((16, 1, 128), jnp.int32), pltpu.SMEM((4, 8, 1, 128), jnp.int32), vm((2, 1, 128), jnp.int32), pltpu.SMEM((2, 1, 128), jnp.int32),
            *[vm((4, 8, HALF, n, 128), F32) for _ in range(4) for n in sizes],
            *[vm((NZ, NC, NX, CAP, n, 128), F32) for n in sizes],
            *[vm((3, 64, n, 128), F32) for n in sizes],
            *[vm((NY, 64, n, 128), F32) for n in sizes],
            vm((4, 256, 256), F32), vm((4, 256, 128), F32), vm((4, 256, 128), F32),
            vm((4, 256, 256), F32), vm((4, 2, 256), F32),
            *[dma(()) for _ in range(13)], dma((NCH, 2)), dma(()), dma((NCH, 2)), dma(()), dma((NCH,)), dma((4,)), *[dma(()) for _ in range(4)],
        ],
        compiler_params=pltpu.CompilerParams(collective_id=0, has_side_effects=True, vmem_limit_bytes=58 * 2**20),
    )(ids, query, slab)


def per_device(slab, queries, block_ids):
    query_count, width_part = queries.shape
    full_width = width_part * lax.axis_size("pb")
    blocks_each = slab.shape[0] // BLOCK
    part, vec = main_call(math.sqrt(full_width), block_ids, queries, slab.reshape(blocks_each, BLOCK, width_part))
    own = lax.dynamic_slice_in_dim(vec, lax.axis_index("pb") * 64, 64, 2)
    scores = vec[:, 0]
    gram = part * own[:, 1][:, :, None]
    penalty = gram * jax.nn.sigmoid(scores[:, None, :] - own[:, 0][:, :, None])
    return (scores, gram, penalty)


def solution(mesh):
    return jax.shard_map(
        per_device,
        mesh=mesh,
        in_specs=(P("db", "pb"), P("db", "pb"), P("db", None)),
        out_specs=(P("db", None), P("db", "pb", None), P("db", "pb", None)),
        check_vma=False,
    )
```

```python
import functools
import math

import jax
import jax.numpy as jnp
from jax import lax
from jax.experimental import pallas as pl
from jax.experimental.pallas import tpu as pltpu
from jax.sharding import PartitionSpec as P

BLOCK = 16
CAP = 12
HALF = 6
NZ, NX, NC, NY = 4, 4, 2, 4
EPS = 1e-06
MESH = pl.DeviceIdType.MESH
F32 = jnp.float32
CHUNKS = ((8, 0, 0), (8, 8, 0), (4, 0, 1), (4, 4, 1), (2, 0, 2), (2, 2, 2), (2, 4, 2), (2, 6, 2))
NCH = len(CHUNKS)
STEPS = ((1, 1), (2, 0), (1, 2), (2, 1), (1, 3), (3, 0), (2, 2), (1, 4), (3, 1), ("wait", 0), (2, 3), (1, 5), (3, 2), (2, 4), (1, 6), ("wait", 1),
         ("sum", 0, 0), ("sum", 0, 1), (3, 3), (2, 5), (1, 7), ("sum", 0, 2), (3, 4), (2, 6), ("sum", 0, 3), ("wait", 2), ("wait", 3), (3, 5),
         (2, 7), ("sum", 1, 0), ("sum", 1, 1), (3, 6), ("sum", 1, 2), ("sum", 1, 3), (3, 7))
FAR = (1, 3, 2)
WIDE = ((1, 0), (3, 0), (1, 1), (3, 1), (2, 0), (2, 1), (0, 1))


def main_kernel(scale, ids, query, slab, part_out, vec_out, slabv, idv, qall, qrow, tab, near, far, nsm, fsm, pos, psm, *rest):
    src_a, mid_a, src_b, mid_b, fin, ysend, cand = (rest[i * NCH:(i + 1) * NCH] for i in range(7))
    (acc, sq, dt, gsend, ssend,
     lsem, isem, psem, nsem, fsem, qsem, ts1, tr1, ts2, tr2, qs, qr, s1s, s1r, s2s, s2r, ys, yr, zr, gs, gr, ss, sr) = rest[7 * NCH:]
    y = lax.axis_index("pb")
    db = lax.axis_index("db")
    z, x, c = db // (NX * NC), (db // NC) % NX, db % NC
    jx = x * NC + c
    jz = z * NC + c

    def dev(yy, zz, xx, cc):
        return (yy, (zz * NX + xx) * NC + cc)

    def up(v, d, n):
        return (v + d) % n

    peers = [dev(y, *at, up(c, e, NC)) for d, e in WIDE if d for at in ((up(z, d, NZ), x), (z, up(x, d, NX)))]
    peers[4:4] = [dev(up(y, d, NY), z, x, c) for d in FAR]
    peers.append(dev(y, z, x, up(c, 1, NC)))
    barrier = pltpu.get_barrier_semaphore()
    for p in peers:
        pl.semaphore_signal(barrier, inc=1, device_id=p, device_id_type=MESH)
    icopy = pltpu.make_async_copy(ids, idv, isem)
    icopy.start()
    qcopy = pltpu.make_async_copy(query, qall.at[y], qsem)
    qcopy.start()
    load = pltpu.make_async_copy(slab, slabv, lsem)
    load.start()

    icopy.wait()
    wide = jnp.concatenate([idv[...]] * 8, axis=1)
    sub = lax.broadcasted_iota(jnp.int32, (16, 128), 0)
    lan = lax.broadcasted_iota(jnp.int32, (16, 128), 1)
    wide = jnp.where(lan // 16 == sub % 8, wide, 0)
    row = [jnp.sum(wide[8 * i:8 * i + 8], axis=0, keepdims=True) for i in range(2)]
    big_r = lax.broadcasted_iota(jnp.int32, (128, 128), 0)
    big_c = lax.broadcasted_iota(jnp.int32, (128, 128), 1)

    def column(v):
        return jnp.broadcast_to(v, (128, 128)).T

    each = slab.shape[0]
    own = [v // each for v in row]
    own_t = [column(v) for v in own]
    rank = [jnp.sum(jnp.where((own_t[0] == own[0]) & (big_r < big_c), 1, 0), axis=0, keepdims=True),
            jnp.sum(jnp.where(own_t[0] == own[1], 1, 0), axis=0, keepdims=True)
            + jnp.sum(jnp.where((own_t[1] == own[1]) & (big_r < big_c), 1, 0), axis=0, keepdims=True)]
    code_t = [column((own[i] * 16 + rank[i]) * each + row[i] % each) for i in range(2)]
    for zz in range(NZ):
        tab[zz] = sum(jnp.sum(jnp.where(code_t[i] // each == big_c + 128 * zz, code_t[i] % each, 0), axis=0, keepdims=True)
                      for i in range(2))
    for i in range(2):
        o = own[i]
        pos[i] = (((o // 8) * NC + o % 2) * NX + (o // 2) % 4) * CAP + rank[i]
    pcopy = pltpu.make_async_copy(pos, psm, psem)
    pcopy.start()
    near[z * NC + c] = tab[z]
    near[8 + jx] = tab[z]
    near[8 + x * NC + 1 - c] = tab[z]

    pl.semaphore_wait(barrier, len(peers))

    def copy(src, dst, ssem, rsem, target):
        return pltpu.make_async_remote_copy(src_ref=src, dst_ref=dst, send_sem=ssem, recv_sem=rsem,
                                            device_id=target, device_id_type=MESH)

    def remote(*args):
        copy(*args).start()

    def arrived(view, sem):
        copy(view, view, sem, sem, peers[0]).wait_recv()

    def left(view, sem):
        copy(view, view, sem, sem, peers[0]).wait_send()

    for d, e in WIDE:
        z2, c2 = up(z, d, NZ), up(c, e, NC)
        remote(tab.at[z2], near.at[z * NC + c], ts1, tr1, dev(y, z2, x, c2))
        if d:
            x2 = up(x, d, NX)
            remote(tab.at[z], near.at[8 + jx], ts1, tr1, dev(y, z, x2, c2))
    arrived(near.at[0:13], tr1)
    ncopy = pltpu.make_async_copy(near, nsm, nsem)
    ncopy.start()
    for d in FAR:
        remote(near.at[0:8], far.at[x], ts2, tr2, dev(y, z, up(x, d, NX), c))
    far[x] = near[0:8]
    load.wait()
    ncopy.wait()

    def tile(ch, at):
        n, r0, kind = CHUNKS[ch]
        if kind == 0:
            return slabv[at, r0:r0 + n, 0:128]
        top = slabv[at, r0:r0 + n, 128:256]
        low = slabv[at, 8 + r0:8 + r0 + n, 128:256]
        left = lax.broadcasted_iota(jnp.int32, (n, 128), 1) < 64
        if kind == 1:
            return jnp.where(left, top, pltpu.roll(low, 64, 1))
        return jnp.where(left, pltpu.roll(top, 64, 1), low)

    def fill(ch, to, at, row, first):
        for s in range(HALF):
            to[ch][(*at, s)] = tile(ch, row(jx * 16 + first + s))

    def gather(ch):
        for d in range(4):
            z2, x2 = up(z, d, NZ), up(x, d, NX)

            def body(j, carry):
                fill(ch, src_a if d else mid_a, (z2, j), lambda k: fsm[j // NC, z2 * NC + j % NC, 0, k], 0)
                fill(ch, src_b if d else mid_b, (x2, j), lambda k: fsm[x2, j, 0, k], HALF)
                return carry

            lax.fori_loop(0, 8, body, 0)

    def open_near():
        for d in range(4):
            z2, x2 = up(z, d, NZ), up(x, d, NX)
            line = (8 + x2 * NC) if d else z * NC

            def body(e, carry):
                if d:
                    fill(0, src_a, (z2, x * NC + e), lambda k: nsm[z2 * NC + e, 0, k], 0)
                    fill(0, src_b, (x2, z * NC + e), lambda k: nsm[line + e, 0, k], HALF)
                fill(0, mid_a, (z, x2 * NC + e), lambda k: nsm[line + e, 0, k], 0)
                fill(0, mid_b, (x, z2 * NC + e), lambda k: nsm[z2 * NC + e, 0, k], HALF)
                return carry

            lax.fori_loop(0, 2, body, 0)
        for d in FAR:
            z2, x2 = up(z, d, NZ), up(x, d, NX)
            mine_a, mine_b = pl.ds(x * NC, NC), pl.ds(z * NC, NC)
            remote(src_a[0].at[z2, mine_a], mid_a[0].at[z, mine_a], s1s, s1r.at[0, 0], dev(y, z2, x, c))
            remote(src_b[0].at[x2, mine_b], mid_b[0].at[x, mine_b], s1s, s1r.at[0, 1], dev(y, z, x2, c))
        for d, e in WIDE:
            z2, x2, c2 = up(z, d, NZ), up(x, d, NX), up(c, e, NC)
            remote(mid_a[0].at[z, x2 * NC + c2], fin[0].at[z, c, x, 0:HALF], s2s, s2r.at[0, 0], dev(y, z, x2, c2))
            remote(mid_b[0].at[x, z2 * NC + c2], fin[0].at[z, c, x, HALF:CAP], s2s, s2r.at[0, 1], dev(y, z2, x, c2))

    def open_far():
        for d in range(1, 4):
            z2, x2 = up(z, d, NZ), up(x, d, NX)

            def body(i, carry):
                k2, e = up(i // NC, 1, 4), i % NC
                z3, x3 = up(z, k2, NZ), up(x, k2, NX)
                fill(0, src_a, (z2, x3 * NC + e), lambda k: fsm[x3, z2 * NC + e, 0, k], 0)
                fill(0, src_b, (x2, z3 * NC + e), lambda k: fsm[x2, z3 * NC + e, 0, k], HALF)
                return carry

            lax.fori_loop(0, 6, body, 0)
        for d in FAR:
            for k2 in range(1, 4):
                z2, x2 = up(z, d, NZ), up(x, d, NX)
                their_a, their_b = pl.ds(up(x, k2, NX) * NC, NC), pl.ds(up(z, k2, NZ) * NC, NC)
                remote(src_a[0].at[z2, their_a], mid_a[0].at[z, their_a], s1s, s1r.at[0, 0], dev(y, z2, x, c))
                remote(src_b[0].at[x2, their_b], mid_b[0].at[x, their_b], s1s, s1r.at[0, 1], dev(y, z, x2, c))

    def stage1(ch):
        gather(ch)
        for d in FAR:
            z2, x2 = up(z, d, NZ), up(x, d, NX)
            remote(src_a[ch].at[z2], mid_a[ch].at[z], s1s, s1r.at[ch, 0], dev(y, z2, x, c))
            remote(src_b[ch].at[x2], mid_b[ch].at[x], s1s, s1r.at[ch, 1], dev(y, z, x2, c))

    def stage2(ch):
        arrived(mid_a[ch].at[0:3], s1r.at[ch, 0])
        arrived(mid_b[ch].at[0:3], s1r.at[ch, 1])
        for d, e in WIDE:
            z2, x2, c2 = up(z, d, NZ), up(x, d, NX), up(c, e, NC)
            if ch:
                remote(mid_a[ch].at[:, x2 * NC + c2], fin[ch].at[:, c, x, 0:HALF], s2s, s2r.at[ch, 0], dev(y, z, x2, c2))
                remote(mid_b[ch].at[:, z2 * NC + c2], fin[ch].at[z, c, :, HALF:CAP], s2s, s2r.at[ch, 1], dev(y, z2, x, c2))
            else:
                for k2 in range(1, 4):
                    z3, x3 = up(z, k2, NZ), up(x, k2, NX)
                    remote(mid_a[0].at[z3, x2 * NC + c2], fin[0].at[z3, c, x, 0:HALF], s2s, s2r.at[0, 0], dev(y, z, x2, c2))
                    remote(mid_b[0].at[x3, z2 * NC + c2], fin[0].at[z, c, x3, HALF:CAP], s2s, s2r.at[0, 1], dev(y, z2, x, c2))
        for i in range(4):
            fin[ch][i, c, x, 0:HALF] = mid_a[ch][i, jx]
            fin[ch][z, c, i, HALF:CAP] = mid_b[ch][i, jz]

    def both_arrived(ch):
        arrived(mid_a[ch].at[:, 0:7], s2r.at[ch, 0])
        arrived(mid_b[ch].at[:, 0:7], s2r.at[ch, 1])

    def pick(ch, y2, q, out):
        flat = fin[ch].reshape(NZ * NC * NX * CAP, CHUNKS[ch][0], 128)
        upper = y2 // 2
        base = (y2 % 2) * 64 + q * 16
        for u in range(16):
            out[q * 16 + u] = flat[psm[upper, 0, base + u]]

    def across(ch):
        both_arrived(ch)
        for d in (*FAR, 0):
            y2 = up(y, d, NY)
            out = ysend[ch].at[d - 1] if d else cand[ch].at[y]

            def body(q, carry):
                pick(ch, y2, q, out)
                return carry

            lax.fori_loop(0, 4, body, 0)
            if d:
                remote(out, cand[ch].at[y], ys, yr.at[ch], dev(y2, z, x, c))

    def across_last(ch):
        both_arrived(ch)
        for q in range(4):
            mine = pl.ds(q * 16, 16)
            for d in (*FAR, 0):
                y2 = up(y, d, NY)
                out = ysend[ch].at[d - 1] if d else cand[ch].at[y]
                pick(ch, y2, q, out)
                if d:
                    remote(out.at[mine], cand[ch].at[y, mine], ys, zr.at[q], dev(y2, z, x, c))

    def nt(a, b):
        return lax.dot_general(a, b, (((1,), (1,)), ((), ())), preferred_element_type=F32)

    left16 = lax.broadcasted_iota(jnp.int32, (16, 8, 128), 2) < 64

    def swap(v):
        return pltpu.roll(v, 64, v.ndim - 1)

    def operands(q, kind):
        mine = pl.ds(q * 16, 16)
        if kind == 0:
            return [jnp.stack([cand[0][yy, mine], cand[1][yy, mine]], axis=1).reshape(256, 128) for yy in range(NY)]
        out = []
        for yy in range(0, NY, 2):
            a, b = (jnp.concatenate([cand[ch][t, mine] for ch in range(NCH) if CHUNKS[ch][2] == kind], axis=1) for t in (yy, yy + 1))
            top = jnp.where(left16, a, swap(b))
            low = jnp.where(left16, swap(a), b)
            out.append(jnp.stack([top, low], axis=1).reshape(256, 128))
        return out

    def partial(q, kind):
        s2 = jnp.zeros((256, 128), F32)
        dd = jnp.zeros((256, 128), F32)
        g = jnp.zeros((256, 256), F32)
        xs = operands(q, kind)
        at = (0, 4, 6)[kind]
        for k in range(0, len(xs), 2):
            his, los = [], []
            for t in (k, k + 1):
                v = xs[t]
                s2 = s2 + v * v
                dd = dd + v * qrow[q, at + t:at + t + 1, :]
                hi = v.astype(jnp.bfloat16)
                his.append(hi)
                los.append((v - hi.astype(F32)).astype(jnp.bfloat16))
            hi = jnp.concatenate(his, axis=1)
            lo = jnp.concatenate(los, axis=1)
            g = g + (nt(hi, hi) + (nt(hi, lo) + nt(lo, hi)))
        return g, s2, dd

    def query_rows():
        row16 = lax.broadcasted_iota(jnp.int32, (16, 256), 0)
        left = lax.broadcasted_iota(jnp.int32, (1, 128), 1) < 64
        for q in range(4):
            rows = [jnp.sum(jnp.where(row16 == 4 * y + q, qall[yy], 0.0), axis=0, keepdims=True) for yy in range(NY)]
            for yy in range(NY):
                qrow[q, yy:yy + 1, :] = rows[yy][:, 0:128]
            far = [v[:, 128:256] for v in rows]
            for k in range(2):
                qrow[q, 4 + k:5 + k, :] = jnp.where(left, far[2 * k], swap(far[2 * k + 1]))
                qrow[q, 6 + k:7 + k, :] = jnp.where(left, swap(far[2 * k]), far[2 * k + 1])

    open_near()
    arrived(far.at[0:3], tr2)
    fcopy = pltpu.make_async_copy(far, fsm, fsem)
    fcopy.start()
    qcopy.wait()
    for d in range(1, NY):
        remote(qall.at[y], qall.at[y], qs, qr, dev(up(y, d, NY), z, x, c))
    fcopy.wait()
    open_far()
    pcopy.wait()
    for stage, ch, *more in STEPS:
        if stage == 1:
            stage1(ch)
            if ch == 1:
                arrived(qall.at[0:3], qr)
                query_rows()
        elif stage == 2:
            stage2(ch)
        elif stage == 3:
            (across_last if ch == NCH - 1 else across)(ch)
        elif stage == "wait":
            arrived(cand[ch].at[0:3], yr.at[ch])
        else:
            q = more[0]
            g, s2, dd = partial(q, ch)
            acc[q] = g if ch == 0 else acc[q] + g
            sq[q] = s2 if ch == 0 else sq[q] + s2
            dt[q] = dd if ch == 0 else dt[q] + dd
    for ch in range(NCH - 1):
        if CHUNKS[ch][2] == 2:
            arrived(cand[ch].at[0:3], yr.at[ch])

    lane = lax.broadcasted_iota(jnp.int32, (256, 128), 1)
    for q in range(4):
        arrived(cand[NCH - 1].at[0:3, pl.ds(q * 16, 16)], zr.at[q])
        g, s2, dd = partial(q, 2)
        g = g + acc[q]
        gsend[q] = g
        for d in FAR:
            y2 = up(y, d, NY)
            remote(gsend.at[q, pl.ds(y2 * 64, 64)], part_out.at[y * 4 + q], gs, gr, dev(y2, z, x, c))
        part_out[y * 4 + q] = gsend[q, pl.ds(pl.multiple_of(y * 64, 64), 64)]
        rn = 1.0 / jnp.sqrt(jnp.sum(s2 + sq[q], axis=1, keepdims=True) + EPS)
        dots = jnp.sum(dd + dt[q], axis=1, keepdims=True)
        qv = qrow[q]
        qn = jnp.sqrt(jnp.sum(jnp.sum(qv * qv, axis=0, keepdims=True), axis=1, keepdims=True) + EPS)
        score = (scale * dots) * (rn / qn)
        ssend[q] = jnp.where(lane == 0, score, rn).T[0:2, :]
        for d in FAR:
            remote(ssend.at[q], vec_out.at[y * 4 + q], ss, sr, dev(up(y, d, NY), z, x, c))
        vec_out[y * 4 + q] = ssend[q]
    arrived(part_out.at[0:12], gr)
    arrived(vec_out.at[0:12], sr)
    left(part_out.at[0:12], gs)
    left(vec_out.at[0:12], ss)
    left(near.at[0:13], ts1)
    left(far.at[0:3], ts2)
    left(qall.at[0:3], qs)
    left(slabv.at[0:288], s1s)
    left(slabv.at[0:336], s2s)
    left(slabv.at[0:192], ys)


def main_call(scale, ids, query, slab):
    dma = pltpu.SemaphoreType.DMA
    vm = pltpu.VMEM
    vmem = pl.BlockSpec(memory_space=pltpu.VMEM)
    anywhere = pl.BlockSpec(memory_space=pl.ANY)
    sizes = [n for n, _, _ in CHUNKS]
    return pl.pallas_call(
        functools.partial(main_kernel, scale),
        out_shape=(pltpu.VMEM((16, 64, 256), F32), pltpu.VMEM((16, 2, 256), F32)),
        in_specs=[anywhere, anywhere, anywhere],
        out_specs=(vmem, vmem),
        scratch_shapes=[
            vm(slab.shape, F32), vm((16, 16), jnp.int32), vm((NY, 16, 256), F32), vm((4, 8, 128), F32),
            vm((4, 1, 128), jnp.int32), vm((16, 1, 128), jnp.int32), vm((4, 8, 1, 128), jnp.int32),
            pltpu.SMEM((16, 1, 128), jnp.int32), pltpu.SMEM((4, 8, 1, 128), jnp.int32), vm((2, 1, 128), jnp.int32), pltpu.SMEM((2, 1, 128), jnp.int32),
            *[vm((4, 8, HALF, n, 128), F32) for _ in range(4) for n in sizes],
            *[vm((NZ, NC, NX, CAP, n, 128), F32) for n in sizes],
            *[vm((3, 64, n, 128), F32) for n in sizes],
            *[vm((NY, 64, n, 128), F32) for n in sizes],
            vm((4, 256, 256), F32), vm((4, 256, 128), F32), vm((4, 256, 128), F32),
            vm((4, 256, 256), F32), vm((4, 2, 256), F32),
            *[dma(()) for _ in range(13)], dma((NCH, 2)), dma(()), dma((NCH, 2)), dma(()), dma((NCH,)), dma((4,)), *[dma(()) for _ in range(4)],
        ],
        compiler_params=pltpu.CompilerParams(collective_id=0, has_side_effects=True, vmem_limit_bytes=58 * 2**20),
    )(ids, query, slab)


def per_device(slab, queries, block_ids):
    query_count, width_part = queries.shape
    full_width = width_part * lax.axis_size("pb")
    blocks_each = slab.shape[0] // BLOCK
    part, vec = main_call(math.sqrt(full_width), block_ids, queries, slab.reshape(blocks_each, BLOCK, width_part))
    own = lax.dynamic_slice_in_dim(vec, lax.axis_index("pb") * 64, 64, 2)
    scores = vec[:, 0]
    gram = part * (own[:, 1][:, :, None] * vec[:, 1][:, None, :])
    penalty = gram * jax.nn.sigmoid(scores[:, None, :] - own[:, 0][:, :, None])
    return (scores, gram, penalty)


def solution(mesh):
    return jax.shard_map(
        per_device,
        mesh=mesh,
        in_specs=(P("db", "pb"), P("db", "pb"), P("db", None)),
        out_specs=(P("db", None), P("db", "pb", None), P("db", "pb", None)),
        check_vma=False,
    )
```

```python
import functools
import math

import jax
import jax.numpy as jnp
from jax import lax
from jax.experimental import pallas as pl
from jax.experimental.pallas import tpu as pltpu
from jax.sharding import PartitionSpec as P

BLOCK = 16
CAP = 12
HALF = 6
NZ, NX, NC, NY = 4, 4, 2, 4
EPS = 1e-06
MESH = pl.DeviceIdType.MESH
F32 = jnp.float32
CHUNKS = ((8, 0, 0), (8, 8, 0), (4, 0, 1), (4, 4, 1), (2, 0, 2), (2, 2, 2), (2, 4, 2), (2, 6, 2))
NCH = len(CHUNKS)
STEPS = ((1, 1), (2, 0), (1, 2), (2, 1), (1, 3), (3, 0), (2, 2), (1, 4), (3, 1), ("wait", 0), (2, 3), (1, 5), (3, 2), (2, 4), (1, 6), ("wait", 1),
         ("sum", 0, 0), ("sum", 0, 1), (3, 3), (2, 5), (1, 7), ("sum", 0, 2), (3, 4), (2, 6), ("sum", 0, 3), ("wait", 2), ("wait", 3), (3, 5),
         (2, 7), ("sum", 1, 0), ("sum", 1, 1), (3, 6), ("sum", 1, 2), ("sum", 1, 3), (3, 7))
FAR = (1, 3, 2)
WIDE = ((1, 0), (3, 0), (1, 1), (3, 1), (2, 0), (2, 1), (0, 1))


def main_kernel(scale, ids, query, slab, part_out, vec_out, slabv, idv, qall, qrow, tab, near, far, nsm, fsm, pos, psm, *rest):
    src_a, mid_a, src_b, mid_b, fin, ysend, cand = (rest[i * NCH:(i + 1) * NCH] for i in range(7))
    (acc, sq, dt, gsend, ssend,
     lsem, isem, psem, nsem, fsem, qsem, ts1, tr1, ts2, tr2, qs, qr, s1s, s1r, s2s, s2r, ys, yr, zr, gs, gr, ss, sr) = rest[7 * NCH:]
    y = lax.axis_index("pb")
    db = lax.axis_index("db")
    z, x, c = db // (NX * NC), (db // NC) % NX, db % NC
    jx = x * NC + c
    jz = z * NC + c

    def dev(yy, zz, xx, cc):
        return (yy, (zz * NX + xx) * NC + cc)

    def up(v, d, n):
        return (v + d) % n

    icopy = pltpu.make_async_copy(ids, idv, isem)
    icopy.start()
    peers = [dev(y, *at, up(c, e, NC)) for d, e in WIDE if d for at in ((up(z, d, NZ), x), (z, up(x, d, NX)))]
    peers[4:4] = [dev(up(y, d, NY), z, x, c) for d in FAR]
    peers.append(dev(y, z, x, up(c, 1, NC)))
    barrier = pltpu.get_barrier_semaphore()
    for p in peers:
        pl.semaphore_signal(barrier, inc=1, device_id=p, device_id_type=MESH)
    qcopy = pltpu.make_async_copy(query, qall.at[y], qsem)
    qcopy.start()
    load = pltpu.make_async_copy(slab, slabv, lsem)
    load.start()

    icopy.wait()
    wide = jnp.concatenate([idv[...]] * 8, axis=1)
    sub = lax.broadcasted_iota(jnp.int32, (16, 128), 0)
    lan = lax.broadcasted_iota(jnp.int32, (16, 128), 1)
    wide = jnp.where(lan // 16 == sub % 8, wide, 0)
    row = [jnp.sum(wide[8 * i:8 * i + 8], axis=0, keepdims=True) for i in range(2)]
    big_r = lax.broadcasted_iota(jnp.int32, (128, 128), 0)
    big_c = lax.broadcasted_iota(jnp.int32, (128, 128), 1)

    def column(v):
        return jnp.broadcast_to(v, (128, 128)).T

    each = slab.shape[0]
    own = [v // each for v in row]
    own_t = [column(v) for v in own]
    rank = [jnp.sum(jnp.where((own_t[0] == own[0]) & (big_r < big_c), 1, 0), axis=0, keepdims=True),
            jnp.sum(jnp.where(own_t[0] == own[1], 1, 0), axis=0, keepdims=True)
            + jnp.sum(jnp.where((own_t[1] == own[1]) & (big_r < big_c), 1, 0), axis=0, keepdims=True)]
    code_t = [column((own[i] * 16 + rank[i]) * each + row[i] % each) for i in range(2)]
    for zz in range(NZ):
        tab[zz] = sum(jnp.sum(jnp.where(code_t[i] // each == big_c + 128 * zz, code_t[i] % each, 0), axis=0, keepdims=True)
                      for i in range(2))
    for i in range(2):
        o = own[i]
        pos[i] = (((o // 8) * NC + o % 2) * NX + (o // 2) % 4) * CAP + rank[i]
    pcopy = pltpu.make_async_copy(pos, psm, psem)
    pcopy.start()
    near[z * NC + c] = tab[z]
    near[8 + jx] = tab[z]
    near[8 + x * NC + 1 - c] = tab[z]

    pl.semaphore_wait(barrier, len(peers))

    def copy(src, dst, ssem, rsem, target):
        return pltpu.make_async_remote_copy(src_ref=src, dst_ref=dst, send_sem=ssem, recv_sem=rsem,
                                            device_id=target, device_id_type=MESH)

    def remote(*args):
        copy(*args).start()

    def arrived(view, sem):
        copy(view, view, sem, sem, peers[0]).wait_recv()

    def left(view, sem):
        copy(view, view, sem, sem, peers[0]).wait_send()

    for d, e in WIDE:
        z2, c2 = up(z, d, NZ), up(c, e, NC)
        remote(tab.at[z2], near.at[z * NC + c], ts1, tr1, dev(y, z2, x, c2))
        if d:
            x2 = up(x, d, NX)
            remote(tab.at[z], near.at[8 + jx], ts1, tr1, dev(y, z, x2, c2))
    arrived(near.at[0:13], tr1)
    ncopy = pltpu.make_async_copy(near, nsm, nsem)
    ncopy.start()
    for d in FAR:
        remote(near.at[0:8], far.at[x], ts2, tr2, dev(y, z, up(x, d, NX), c))
    far[x] = near[0:8]
    load.wait()
    ncopy.wait()

    def tile(ch, at):
        n, r0, kind = CHUNKS[ch]
        if kind == 0:
            return slabv[at, r0:r0 + n, 0:128]
        top = slabv[at, r0:r0 + n, 128:256]
        low = slabv[at, 8 + r0:8 + r0 + n, 128:256]
        left = lax.broadcasted_iota(jnp.int32, (n, 128), 1) < 64
        if kind == 1:
            return jnp.where(left, top, pltpu.roll(low, 64, 1))
        return jnp.where(left, pltpu.roll(top, 64, 1), low)

    def fill(ch, to, at, row, first):
        for s in range(HALF):
            to[ch][(*at, s)] = tile(ch, row(jx * 16 + first + s))

    def gather(ch):
        for d in range(4):
            z2, x2 = up(z, d, NZ), up(x, d, NX)

            def body(j, carry):
                fill(ch, src_a if d else mid_a, (z2, j), lambda k: fsm[j // NC, z2 * NC + j % NC, 0, k], 0)
                fill(ch, src_b if d else mid_b, (x2, j), lambda k: fsm[x2, j, 0, k], HALF)
                return carry

            lax.fori_loop(0, 8, body, 0)

    def open_near():
        for d in range(4):
            z2, x2 = up(z, d, NZ), up(x, d, NX)
            line = (8 + x2 * NC) if d else z * NC

            def body(e, carry):
                if d:
                    fill(0, src_a, (z2, x * NC + e), lambda k: nsm[z2 * NC + e, 0, k], 0)
                    fill(0, src_b, (x2, z * NC + e), lambda k: nsm[line + e, 0, k], HALF)
                fill(0, mid_a, (z, x2 * NC + e), lambda k: nsm[line + e, 0, k], 0)
                fill(0, mid_b, (x, z2 * NC + e), lambda k: nsm[z2 * NC + e, 0, k], HALF)
                return carry

            lax.fori_loop(0, 2, body, 0)
        for d in FAR:
            z2, x2 = up(z, d, NZ), up(x, d, NX)
            mine_a, mine_b = pl.ds(x * NC, NC), pl.ds(z * NC, NC)
            remote(src_a[0].at[z2, mine_a], mid_a[0].at[z, mine_a], s1s, s1r.at[0], dev(y, z2, x, c))
            remote(src_b[0].at[x2, mine_b], mid_b[0].at[x, mine_b], s1s, s1r.at[0], dev(y, z, x2, c))
        for d, e in WIDE:
            z2, x2, c2 = up(z, d, NZ), up(x, d, NX), up(c, e, NC)
            remote(mid_a[0].at[z, x2 * NC + c2], fin[0].at[z, c, x, 0:HALF], s2s, s2r.at[0], dev(y, z, x2, c2))
            remote(mid_b[0].at[x, z2 * NC + c2], fin[0].at[z, c, x, HALF:CAP], s2s, s2r.at[0], dev(y, z2, x, c2))

    def open_far():
        for d in range(1, 4):
            z2, x2 = up(z, d, NZ), up(x, d, NX)

            def body(i, carry):
                k2, e = up(i // NC, 1, 4), i % NC
                z3, x3 = up(z, k2, NZ), up(x, k2, NX)
                fill(0, src_a, (z2, x3 * NC + e), lambda k: fsm[x3, z2 * NC + e, 0, k], 0)
                fill(0, src_b, (x2, z3 * NC + e), lambda k: fsm[x2, z3 * NC + e, 0, k], HALF)
                return carry

            lax.fori_loop(0, 6, body, 0)
        for d in FAR:
            for k2 in range(1, 4):
                z2, x2 = up(z, d, NZ), up(x, d, NX)
                their_a, their_b = pl.ds(up(x, k2, NX) * NC, NC), pl.ds(up(z, k2, NZ) * NC, NC)
                remote(src_a[0].at[z2, their_a], mid_a[0].at[z, their_a], s1s, s1r.at[0], dev(y, z2, x, c))
                remote(src_b[0].at[x2, their_b], mid_b[0].at[x, their_b], s1s, s1r.at[0], dev(y, z, x2, c))

    def stage1(ch):
        gather(ch)
        for d in FAR:
            z2, x2 = up(z, d, NZ), up(x, d, NX)
            remote(src_a[ch].at[z2], mid_a[ch].at[z], s1s, s1r.at[ch], dev(y, z2, x, c))
            remote(src_b[ch].at[x2], mid_b[ch].at[x], s1s, s1r.at[ch], dev(y, z, x2, c))

    def stage2(ch):
        arrived(slabv.at[0:9 * CHUNKS[ch][0]], s1r.at[ch])
        for d, e in WIDE:
            z2, x2, c2 = up(z, d, NZ), up(x, d, NX), up(c, e, NC)
            if ch:
                remote(mid_a[ch].at[:, x2 * NC + c2], fin[ch].at[:, c, x, 0:HALF], s2s, s2r.at[ch], dev(y, z, x2, c2))
                remote(mid_b[ch].at[:, z2 * NC + c2], fin[ch].at[z, c, :, HALF:CAP], s2s, s2r.at[ch], dev(y, z2, x, c2))
            else:
                for k2 in range(1, 4):
                    z3, x3 = up(z, k2, NZ), up(x, k2, NX)
                    remote(mid_a[0].at[z3, x2 * NC + c2], fin[0].at[z3, c, x, 0:HALF], s2s, s2r.at[0], dev(y, z, x2, c2))
                    remote(mid_b[0].at[x3, z2 * NC + c2], fin[0].at[z, c, x3, HALF:CAP], s2s, s2r.at[0], dev(y, z2, x, c2))
        for i in range(4):
            fin[ch][i, c, x, 0:HALF] = mid_a[ch][i, jx]
            fin[ch][z, c, i, HALF:CAP] = mid_b[ch][i, jz]

    def both_arrived(ch):
        arrived(slabv.at[0:21 * CHUNKS[ch][0] // 2], s2r.at[ch])

    def pick(ch, y2, q, out):
        flat = fin[ch].reshape(NZ * NC * NX * CAP, CHUNKS[ch][0], 128)
        upper = y2 // 2
        base = (y2 % 2) * 64 + q * 16
        for u in range(16):
            out[q * 16 + u] = flat[psm[upper, 0, base + u]]

    def across(ch):
        both_arrived(ch)
        for d in (*FAR, 0):
            y2 = up(y, d, NY)
            out = ysend[ch].at[d - 1] if d else cand[ch].at[y]

            def body(q, carry):
                pick(ch, y2, q, out)
                return carry

            lax.fori_loop(0, 4, body, 0)
            if d:
                remote(out, cand[ch].at[y], ys, yr.at[ch], dev(y2, z, x, c))

    def across_last(ch):
        both_arrived(ch)
        for q in range(4):
            mine = pl.ds(q * 16, 16)
            for d in (*FAR, 0):
                y2 = up(y, d, NY)
                out = ysend[ch].at[d - 1] if d else cand[ch].at[y]
                pick(ch, y2, q, out)
                if d:
                    remote(out.at[mine], cand[ch].at[y, mine], ys, zr.at[q], dev(y2, z, x, c))

    def nt(a, b):
        return lax.dot_general(a, b, (((1,), (1,)), ((), ())), preferred_element_type=F32)

    left16 = lax.broadcasted_iota(jnp.int32, (16, 8, 128), 2) < 64

    def swap(v):
        return pltpu.roll(v, 64, v.ndim - 1)

    def operands(q, kind):
        mine = pl.ds(q * 16, 16)
        if kind == 0:
            return [jnp.stack([cand[0][yy, mine], cand[1][yy, mine]], axis=1).reshape(256, 128) for yy in range(NY)]
        out = []
        for yy in range(0, NY, 2):
            a, b = (jnp.concatenate([cand[ch][t, mine] for ch in range(NCH) if CHUNKS[ch][2] == kind], axis=1) for t in (yy, yy + 1))
            top = jnp.where(left16, a, swap(b))
            low = jnp.where(left16, swap(a), b)
            out.append(jnp.stack([top, low], axis=1).reshape(256, 128))
        return out

    def partial(q, kind):
        s2 = jnp.zeros((256, 128), F32)
        dd = jnp.zeros((256, 128), F32)
        g = jnp.zeros((256, 256), F32)
        xs = operands(q, kind)
        at = (0, 4, 6)[kind]
        for k in range(0, len(xs), 2):
            his, los = [], []
            for t in (k, k + 1):
                v = xs[t]
                s2 = s2 + v * v
                dd = dd + v * qrow[q, at + t:at + t + 1, :]
                hi = v.astype(jnp.bfloat16)
                his.append(hi)
                los.append((v - hi.astype(F32)).astype(jnp.bfloat16))
            hi = jnp.concatenate(his, axis=1)
            lo = jnp.concatenate(los, axis=1)
            g = g + (nt(hi, hi) + (nt(hi, lo) + nt(lo, hi)))
        return g, s2, dd

    def query_rows():
        row16 = lax.broadcasted_iota(jnp.int32, (16, 256), 0)
        left = lax.broadcasted_iota(jnp.int32, (1, 128), 1) < 64
        for q in range(4):
            rows = [jnp.sum(jnp.where(row16 == 4 * y + q, qall[yy], 0.0), axis=0, keepdims=True) for yy in range(NY)]
            for yy in range(NY):
                qrow[q, yy:yy + 1, :] = rows[yy][:, 0:128]
            far = [v[:, 128:256] for v in rows]
            for k in range(2):
                qrow[q, 4 + k:5 + k, :] = jnp.where(left, far[2 * k], swap(far[2 * k + 1]))
                qrow[q, 6 + k:7 + k, :] = jnp.where(left, swap(far[2 * k]), far[2 * k + 1])

    open_near()
    arrived(far.at[0:3], tr2)
    fcopy = pltpu.make_async_copy(far, fsm, fsem)
    fcopy.start()
    qcopy.wait()
    for d in range(1, NY):
        remote(qall.at[y], qall.at[y], qs, qr, dev(up(y, d, NY), z, x, c))
    fcopy.wait()
    open_far()
    pcopy.wait()
    for stage, ch, *more in STEPS:
        if stage == 1:
            stage1(ch)
            if ch == 1:
                arrived(qall.at[0:3], qr)
                query_rows()
        elif stage == 2:
            stage2(ch)
        elif stage == 3:
            (across_last if ch == NCH - 1 else across)(ch)
        elif stage == "wait":
            arrived(cand[ch].at[0:3], yr.at[ch])
        else:
            q = more[0]
            g, s2, dd = partial(q, ch)
            acc[q] = g if ch == 0 else acc[q] + g
            sq[q] = s2 if ch == 0 else sq[q] + s2
            dt[q] = dd if ch == 0 else dt[q] + dd
    for ch in range(NCH - 1):
        if CHUNKS[ch][2] == 2:
            arrived(cand[ch].at[0:3], yr.at[ch])

    lane = lax.broadcasted_iota(jnp.int32, (256, 128), 1)
    for q in range(4):
        arrived(cand[NCH - 1].at[0:3, pl.ds(q * 16, 16)], zr.at[q])
        g, s2, dd = partial(q, 2)
        g = g + acc[q]
        gsend[q] = g
        for d in FAR:
            y2 = up(y, d, NY)
            remote(gsend.at[q, pl.ds(y2 * 64, 64)], part_out.at[y * 4 + q], gs, gr, dev(y2, z, x, c))
        part_out[y * 4 + q] = gsend[q, pl.ds(pl.multiple_of(y * 64, 64), 64)]
        rn = 1.0 / jnp.sqrt(jnp.sum(s2 + sq[q], axis=1, keepdims=True) + EPS)
        dots = jnp.sum(dd + dt[q], axis=1, keepdims=True)
        qv = qrow[q]
        qn = jnp.sqrt(jnp.sum(jnp.sum(qv * qv, axis=0, keepdims=True), axis=1, keepdims=True) + EPS)
        score = (scale * dots) * (rn / qn)
        ssend[q] = jnp.where(lane == 0, score, rn).T[0:2, :]
        for d in FAR:
            remote(ssend.at[q], vec_out.at[y * 4 + q], ss, sr, dev(up(y, d, NY), z, x, c))
        vec_out[y * 4 + q] = ssend[q]
    arrived(part_out.at[0:12], gr)
    arrived(vec_out.at[0:12], sr)
    left(part_out.at[0:12], gs)
    left(vec_out.at[0:12], ss)
    left(near.at[0:13], ts1)
    left(far.at[0:3], ts2)
    left(qall.at[0:3], qs)
    left(slabv.at[0:288], s1s)
    left(slabv.at[0:336], s2s)
    left(slabv.at[0:192], ys)


def main_call(scale, ids, query, slab):
    dma = pltpu.SemaphoreType.DMA
    vm = pltpu.VMEM
    vmem = pl.BlockSpec(memory_space=pltpu.VMEM)
    anywhere = pl.BlockSpec(memory_space=pl.ANY)
    sizes = [n for n, _, _ in CHUNKS]
    return pl.pallas_call(
        functools.partial(main_kernel, scale),
        out_shape=(pltpu.VMEM((16, 64, 256), F32), pltpu.VMEM((16, 2, 256), F32)),
        in_specs=[anywhere, anywhere, anywhere],
        out_specs=(vmem, vmem),
        scratch_shapes=[
            vm(slab.shape, F32), vm((16, 16), jnp.int32), vm((NY, 16, 256), F32), vm((4, 8, 128), F32),
            vm((4, 1, 128), jnp.int32), vm((16, 1, 128), jnp.int32), vm((4, 8, 1, 128), jnp.int32),
            pltpu.SMEM((16, 1, 128), jnp.int32), pltpu.SMEM((4, 8, 1, 128), jnp.int32), vm((2, 1, 128), jnp.int32), pltpu.SMEM((2, 1, 128), jnp.int32),
            *[vm((4, 8, HALF, n, 128), F32) for _ in range(4) for n in sizes],
            *[vm((NZ, NC, NX, CAP, n, 128), F32) for n in sizes],
            *[vm((3, 64, n, 128), F32) for n in sizes],
            *[vm((NY, 64, n, 128), F32) for n in sizes],
            vm((4, 256, 256), F32), vm((4, 256, 128), F32), vm((4, 256, 128), F32),
            vm((4, 256, 256), F32), vm((4, 2, 256), F32),
            *[dma(()) for _ in range(13)], dma((NCH,)), dma(()), dma((NCH,)), dma(()), dma((NCH,)), dma((4,)), *[dma(()) for _ in range(4)],
        ],
        compiler_params=pltpu.CompilerParams(collective_id=0, has_side_effects=True, vmem_limit_bytes=58 * 2**20),
    )(ids, query, slab)


def per_device(slab, queries, block_ids):
    query_count, width_part = queries.shape
    full_width = width_part * lax.axis_size("pb")
    blocks_each = slab.shape[0] // BLOCK
    part, vec = main_call(math.sqrt(full_width), block_ids, queries, slab.reshape(blocks_each, BLOCK, width_part))
    own = lax.dynamic_slice_in_dim(vec, lax.axis_index("pb") * 64, 64, 2)
    scores = vec[:, 0]
    gram = part * (own[:, 1][:, :, None] * vec[:, 1][:, None, :])
    penalty = gram * jax.nn.sigmoid(scores[:, None, :] - own[:, 0][:, :, None])
    return (scores, gram, penalty)


def solution(mesh):
    return jax.shard_map(
        per_device,
        mesh=mesh,
        in_specs=(P("db", "pb"), P("db", "pb"), P("db", None)),
        out_specs=(P("db", None), P("db", "pb", None), P("db", "pb", None)),
        check_vma=False,
    )
```

```python
import functools
import math

import jax
import jax.numpy as jnp
from jax import lax
from jax.experimental import pallas as pl
from jax.experimental.pallas import tpu as pltpu
from jax.sharding import PartitionSpec as P

BLOCK = 16
CAP = 12
HALF = 6
NZ, NX, NC, NY = 4, 4, 2, 4
EPS = 1e-06
MESH = pl.DeviceIdType.MESH
F32 = jnp.float32
CHUNKS = ((8, 0, 0), (8, 8, 0), (4, 0, 1), (4, 4, 1), (2, 0, 2), (2, 2, 2), (2, 4, 2), (2, 6, 2))
NCH = len(CHUNKS)
STEPS = ((1, 1), (2, 0), (1, 2), (2, 1), (1, 3), (3, 0), (2, 2), (1, 4), (3, 1), ("wait", 0), (2, 3), (1, 5), (3, 2), (2, 4), (1, 6), ("wait", 1),
         ("sum", 0, 0), ("sum", 0, 1), (3, 3), (2, 5), (1, 7), ("sum", 0, 2), (3, 4), (2, 6), ("sum", 0, 3), ("wait", 2), ("wait", 3), (3, 5),
         (2, 7), ("sum", 1, 0), ("sum", 1, 1), (3, 6), ("sum", 1, 2), ("sum", 1, 3), (3, 7))
FAR = (1, 3, 2)
WIDE = ((1, 0), (3, 0), (1, 1), (3, 1), (2, 0), (2, 1), (0, 1))


def main_kernel(scale, ids, query, slab, part_out, vec_out, slabv, idv, qall, qrow, tab, near, far, nsm, fsm, pos, psm, *rest):
    src_a, mid_a, src_b, mid_b, fin, ysend, cand = (rest[i * NCH:(i + 1) * NCH] for i in range(7))
    (acc, sq, dt, gsend, ssend,
     lsem, isem, psem, nsem, fsem, qsem, ts1, tr1, ts2, tr2, qs, qr, s1s, s1r, s2s, s2r, ys, yr, zr, gs, gr, ss, sr) = rest[7 * NCH:]
    y = lax.axis_index("pb")
    db = lax.axis_index("db")
    z, x, c = db // (NX * NC), (db // NC) % NX, db % NC
    jx = x * NC + c
    jz = z * NC + c

    def dev(yy, zz, xx, cc):
        return (yy, (zz * NX + xx) * NC + cc)

    def up(v, d, n):
        return (v + d) % n

    icopy = pltpu.make_async_copy(ids, idv, isem)
    icopy.start()
    peers = [dev(y, *at, up(c, e, NC)) for d, e in WIDE if d for at in ((up(z, d, NZ), x), (z, up(x, d, NX)))]
    peers[4:4] = [dev(up(y, d, NY), z, x, c) for d in FAR]
    peers.append(dev(y, z, x, up(c, 1, NC)))
    barrier = pltpu.get_barrier_semaphore()
    for p in peers:
        pl.semaphore_signal(barrier, inc=1, device_id=p, device_id_type=MESH)
    qcopy = pltpu.make_async_copy(query, qall.at[y], qsem)
    qcopy.start()
    load = pltpu.make_async_copy(slab, slabv, lsem)
    load.start()

    icopy.wait()
    wide = jnp.concatenate([idv[...]] * 8, axis=1)
    sub = lax.broadcasted_iota(jnp.int32, (16, 128), 0)
    lan = lax.broadcasted_iota(jnp.int32, (16, 128), 1)
    wide = jnp.where(lan // 16 == sub % 8, wide, 0)
    row = [jnp.sum(wide[8 * i:8 * i + 8], axis=0, keepdims=True) for i in range(2)]
    big_r = lax.broadcasted_iota(jnp.int32, (128, 128), 0)
    big_c = lax.broadcasted_iota(jnp.int32, (128, 128), 1)

    def column(v):
        return jnp.broadcast_to(v, (128, 128)).T

    each = slab.shape[0]
    own = [v // each for v in row]
    own_t = [column(v) for v in own]
    rank = [jnp.sum(jnp.where((own_t[0] == own[0]) & (big_r < big_c), 1, 0), axis=0, keepdims=True),
            jnp.sum(jnp.where(own_t[0] == own[1], 1, 0), axis=0, keepdims=True)
            + jnp.sum(jnp.where((own_t[1] == own[1]) & (big_r < big_c), 1, 0), axis=0, keepdims=True)]
    code_t = [column((own[i] * 16 + rank[i]) * each + row[i] % each) for i in range(2)]
    for zz in range(NZ):
        tab[zz] = sum(jnp.sum(jnp.where(code_t[i] // each == big_c + 128 * zz, code_t[i] % each, 0), axis=0, keepdims=True)
                      for i in range(2))
    for i in range(2):
        o = own[i]
        pos[i] = (((o // 8) * NC + o % 2) * NX + (o // 2) % 4) * CAP + rank[i]
    pcopy = pltpu.make_async_copy(pos, psm, psem)
    pcopy.start()
    near[z * NC + c] = tab[z]
    near[8 + jx] = tab[z]
    near[8 + x * NC + 1 - c] = tab[z]

    pl.semaphore_wait(barrier, len(peers))

    def copy(src, dst, ssem, rsem, target):
        return pltpu.make_async_remote_copy(src_ref=src, dst_ref=dst, send_sem=ssem, recv_sem=rsem,
                                            device_id=target, device_id_type=MESH)

    def remote(*args):
        copy(*args).start()

    def arrived(view, sem):
        copy(view, view, sem, sem, peers[0]).wait_recv()

    def left(view, sem):
        copy(view, view, sem, sem, peers[0]).wait_send()

    for d, e in WIDE:
        z2, c2 = up(z, d, NZ), up(c, e, NC)
        remote(tab.at[z2], near.at[z * NC + c], ts1, tr1, dev(y, z2, x, c2))
        if d:
            x2 = up(x, d, NX)
            remote(tab.at[z], near.at[8 + jx], ts1, tr1, dev(y, z, x2, c2))
    arrived(near.at[0:13], tr1)
    ncopy = pltpu.make_async_copy(near, nsm, nsem)
    ncopy.start()
    for d in FAR:
        remote(near.at[0:8], far.at[x], ts2, tr2, dev(y, z, up(x, d, NX), c))
    far[x] = near[0:8]
    load.wait()
    ncopy.wait()

    def tile(ch, at):
        n, r0, kind = CHUNKS[ch]
        if kind == 0:
            return slabv[at, r0:r0 + n, 0:128]
        top = slabv[at, r0:r0 + n, 128:256]
        low = slabv[at, 8 + r0:8 + r0 + n, 128:256]
        left = lax.broadcasted_iota(jnp.int32, (n, 128), 1) < 64
        if kind == 1:
            return jnp.where(left, top, pltpu.roll(low, 64, 1))
        return jnp.where(left, pltpu.roll(top, 64, 1), low)

    def fill(ch, to, at, row, first):
        for s in range(HALF):
            to[ch][(*at, s)] = tile(ch, row(jx * 16 + first + s))

    def gather(ch):
        for d in range(4):
            z2, x2 = up(z, d, NZ), up(x, d, NX)

            def body(j, carry):
                fill(ch, src_a if d else mid_a, (z2, j), lambda k: fsm[j // NC, z2 * NC + j % NC, 0, k], 0)
                fill(ch, src_b if d else mid_b, (x2, j), lambda k: fsm[x2, j, 0, k], HALF)
                return carry

            lax.fori_loop(0, 8, body, 0)

    def own_pieces(ch):
        for d, e in WIDE:
            z2, x2, c2 = up(z, d, NZ), up(x, d, NX), up(c, e, NC)
            remote(mid_a[ch].at[z, x2 * NC + c2], fin[ch].at[z, c, x, 0:HALF], s2s, s2r.at[ch], dev(y, z, x2, c2))
            remote(mid_b[ch].at[x, z2 * NC + c2], fin[ch].at[z, c, x, HALF:CAP], s2s, s2r.at[ch], dev(y, z2, x, c2))

    def open_near():
        for d in range(4):
            z2, x2 = up(z, d, NZ), up(x, d, NX)
            line = (8 + x2 * NC) if d else z * NC

            def body(e, carry):
                if d:
                    fill(0, src_a, (z2, x * NC + e), lambda k: nsm[z2 * NC + e, 0, k], 0)
                    fill(0, src_b, (x2, z * NC + e), lambda k: nsm[line + e, 0, k], HALF)
                fill(0, mid_a, (z, x2 * NC + e), lambda k: nsm[line + e, 0, k], 0)
                fill(0, mid_b, (x, z2 * NC + e), lambda k: nsm[z2 * NC + e, 0, k], HALF)
                return carry

            lax.fori_loop(0, 2, body, 0)
        for d in FAR:
            z2, x2 = up(z, d, NZ), up(x, d, NX)
            mine_a, mine_b = pl.ds(x * NC, NC), pl.ds(z * NC, NC)
            remote(src_a[0].at[z2, mine_a], mid_a[0].at[z, mine_a], s1s, s1r.at[0], dev(y, z2, x, c))
            remote(src_b[0].at[x2, mine_b], mid_b[0].at[x, mine_b], s1s, s1r.at[0], dev(y, z, x2, c))
        own_pieces(0)

    def open_far():
        for d in range(1, 4):
            z2, x2 = up(z, d, NZ), up(x, d, NX)

            def body(i, carry):
                k2, e = up(i // NC, 1, 4), i % NC
                z3, x3 = up(z, k2, NZ), up(x, k2, NX)
                fill(0, src_a, (z2, x3 * NC + e), lambda k: fsm[x3, z2 * NC + e, 0, k], 0)
                fill(0, src_b, (x2, z3 * NC + e), lambda k: fsm[x2, z3 * NC + e, 0, k], HALF)
                return carry

            lax.fori_loop(0, 6, body, 0)
        for d in FAR:
            for k2 in range(1, 4):
                z2, x2 = up(z, d, NZ), up(x, d, NX)
                their_a, their_b = pl.ds(up(x, k2, NX) * NC, NC), pl.ds(up(z, k2, NZ) * NC, NC)
                remote(src_a[0].at[z2, their_a], mid_a[0].at[z, their_a], s1s, s1r.at[0], dev(y, z2, x, c))
                remote(src_b[0].at[x2, their_b], mid_b[0].at[x, their_b], s1s, s1r.at[0], dev(y, z, x2, c))

    def stage1(ch):
        gather(ch)
        for d in FAR:
            z2, x2 = up(z, d, NZ), up(x, d, NX)
            remote(src_a[ch].at[z2], mid_a[ch].at[z], s1s, s1r.at[ch], dev(y, z2, x, c))
            remote(src_b[ch].at[x2], mid_b[ch].at[x], s1s, s1r.at[ch], dev(y, z, x2, c))
        if ch == NCH - 1:
            own_pieces(ch)

    def stage2(ch):
        arrived(slabv.at[0:9 * CHUNKS[ch][0]], s1r.at[ch])
        for d, e in WIDE:
            z2, x2, c2 = up(z, d, NZ), up(x, d, NX), up(c, e, NC)
            if ch not in (0, NCH - 1):
                remote(mid_a[ch].at[:, x2 * NC + c2], fin[ch].at[:, c, x, 0:HALF], s2s, s2r.at[ch], dev(y, z, x2, c2))
                remote(mid_b[ch].at[:, z2 * NC + c2], fin[ch].at[z, c, :, HALF:CAP], s2s, s2r.at[ch], dev(y, z2, x, c2))
            else:
                for k2 in range(1, 4):
                    z3, x3 = up(z, k2, NZ), up(x, k2, NX)
                    remote(mid_a[ch].at[z3, x2 * NC + c2], fin[ch].at[z3, c, x, 0:HALF], s2s, s2r.at[ch], dev(y, z, x2, c2))
                    remote(mid_b[ch].at[x3, z2 * NC + c2], fin[ch].at[z, c, x3, HALF:CAP], s2s, s2r.at[ch], dev(y, z2, x, c2))
        for i in range(4):
            fin[ch][i, c, x, 0:HALF] = mid_a[ch][i, jx]
            fin[ch][z, c, i, HALF:CAP] = mid_b[ch][i, jz]

    def both_arrived(ch):
        arrived(slabv.at[0:21 * CHUNKS[ch][0] // 2], s2r.at[ch])

    def pick(ch, y2, q, out):
        flat = fin[ch].reshape(NZ * NC * NX * CAP, CHUNKS[ch][0], 128)
        upper = y2 // 2
        base = (y2 % 2) * 64 + q * 16
        for u in range(16):
            out[q * 16 + u] = flat[psm[upper, 0, base + u]]

    def across(ch):
        both_arrived(ch)
        for d in (*FAR, 0):
            y2 = up(y, d, NY)
            out = ysend[ch].at[d - 1] if d else cand[ch].at[y]

            def body(q, carry):
                pick(ch, y2, q, out)
                return carry

            lax.fori_loop(0, 4, body, 0)
            if d:
                remote(out, cand[ch].at[y], ys, yr.at[ch], dev(y2, z, x, c))

    def across_last(ch):
        both_arrived(ch)
        for q in range(4):
            mine = pl.ds(q * 16, 16)
            for d in (*FAR, 0):
                y2 = up(y, d, NY)
                out = ysend[ch].at[d - 1] if d else cand[ch].at[y]
                pick(ch, y2, q, out)
                if d:
                    remote(out.at[mine], cand[ch].at[y, mine], ys, zr.at[q], dev(y2, z, x, c))

    def nt(a, b):
        return lax.dot_general(a, b, (((1,), (1,)), ((), ())), preferred_element_type=F32)

    left16 = lax.broadcasted_iota(jnp.int32, (16, 8, 128), 2) < 64

    def swap(v):
        return pltpu.roll(v, 64, v.ndim - 1)

    def operands(q, kind):
        mine = pl.ds(q * 16, 16)
        if kind == 0:
            return [jnp.stack([cand[0][yy, mine], cand[1][yy, mine]], axis=1).reshape(256, 128) for yy in range(NY)]
        out = []
        for yy in range(0, NY, 2):
            a, b = (jnp.concatenate([cand[ch][t, mine] for ch in range(NCH) if CHUNKS[ch][2] == kind], axis=1) for t in (yy, yy + 1))
            top = jnp.where(left16, a, swap(b))
            low = jnp.where(left16, swap(a), b)
            out.append(jnp.stack([top, low], axis=1).reshape(256, 128))
        return out

    def partial(q, kind):
        s2 = jnp.zeros((256, 128), F32)
        dd = jnp.zeros((256, 128), F32)
        g = jnp.zeros((256, 256), F32)
        xs = operands(q, kind)
        at = (0, 4, 6)[kind]
        for k in range(0, len(xs), 2):
            his, los = [], []
            for t in (k, k + 1):
                v = xs[t]
                s2 = s2 + v * v
                dd = dd + v * qrow[q, at + t:at + t + 1, :]
                hi = v.astype(jnp.bfloat16)
                his.append(hi)
                los.append((v - hi.astype(F32)).astype(jnp.bfloat16))
            hi = jnp.concatenate(his, axis=1)
            lo = jnp.concatenate(los, axis=1)
            g = g + (nt(hi, hi) + (nt(hi, lo) + nt(lo, hi)))
        return g, s2, dd

    def query_rows():
        row16 = lax.broadcasted_iota(jnp.int32, (16, 256), 0)
        left = lax.broadcasted_iota(jnp.int32, (1, 128), 1) < 64
        for q in range(4):
            rows = [jnp.sum(jnp.where(row16 == 4 * y + q, qall[yy], 0.0), axis=0, keepdims=True) for yy in range(NY)]
            for yy in range(NY):
                qrow[q, yy:yy + 1, :] = rows[yy][:, 0:128]
            far = [v[:, 128:256] for v in rows]
            for k in range(2):
                qrow[q, 4 + k:5 + k, :] = jnp.where(left, far[2 * k], swap(far[2 * k + 1]))
                qrow[q, 6 + k:7 + k, :] = jnp.where(left, swap(far[2 * k]), far[2 * k + 1])

    open_near()
    arrived(far.at[0:3], tr2)
    fcopy = pltpu.make_async_copy(far, fsm, fsem)
    fcopy.start()
    qcopy.wait()
    for d in range(1, NY):
        remote(qall.at[y], qall.at[y], qs, qr, dev(up(y, d, NY), z, x, c))
    fcopy.wait()
    open_far()
    pcopy.wait()
    for stage, ch, *more in STEPS:
        if stage == 1:
            stage1(ch)
            if ch == 1:
                arrived(qall.at[0:3], qr)
                query_rows()
        elif stage == 2:
            stage2(ch)
        elif stage == 3:
            (across_last if ch == NCH - 1 else across)(ch)
        elif stage == "wait":
            arrived(cand[ch].at[0:3], yr.at[ch])
        else:
            q = more[0]
            g, s2, dd = partial(q, ch)
            acc[q] = g if ch == 0 else acc[q] + g
            sq[q] = s2 if ch == 0 else sq[q] + s2
            dt[q] = dd if ch == 0 else dt[q] + dd
    for ch in range(NCH - 1):
        if CHUNKS[ch][2] == 2:
            arrived(cand[ch].at[0:3], yr.at[ch])

    lane = lax.broadcasted_iota(jnp.int32, (256, 128), 1)
    for q in range(4):
        arrived(cand[NCH - 1].at[0:3, pl.ds(q * 16, 16)], zr.at[q])
        g, s2, dd = partial(q, 2)
        g = g + acc[q]
        gsend[q] = g
        for d in FAR:
            y2 = up(y, d, NY)
            remote(gsend.at[q, pl.ds(y2 * 64, 64)], part_out.at[y * 4 + q], gs, gr, dev(y2, z, x, c))
        part_out[y * 4 + q] = gsend[q, pl.ds(pl.multiple_of(y * 64, 64), 64)]
        rn = 1.0 / jnp.sqrt(jnp.sum(s2 + sq[q], axis=1, keepdims=True) + EPS)
        dots = jnp.sum(dd + dt[q], axis=1, keepdims=True)
        qv = qrow[q]
        qn = jnp.sqrt(jnp.sum(jnp.sum(qv * qv, axis=0, keepdims=True), axis=1, keepdims=True) + EPS)
        score = (scale * dots) * (rn / qn)
        ssend[q] = jnp.where(lane == 0, score, rn).T[0:2, :]
        for d in FAR:
            remote(ssend.at[q], vec_out.at[y * 4 + q], ss, sr, dev(up(y, d, NY), z, x, c))
        vec_out[y * 4 + q] = ssend[q]
    arrived(part_out.at[0:12], gr)
    arrived(vec_out.at[0:12], sr)
    left(part_out.at[0:12], gs)
    left(vec_out.at[0:12], ss)
    left(near.at[0:13], ts1)
    left(far.at[0:3], ts2)
    left(qall.at[0:3], qs)
    left(slabv.at[0:288], s1s)
    left(slabv.at[0:336], s2s)
    left(slabv.at[0:192], ys)


def main_call(scale, ids, query, slab):
    dma = pltpu.SemaphoreType.DMA
    vm = pltpu.VMEM
    vmem = pl.BlockSpec(memory_space=pltpu.VMEM)
    anywhere = pl.BlockSpec(memory_space=pl.ANY)
    sizes = [n for n, _, _ in CHUNKS]
    return pl.pallas_call(
        functools.partial(main_kernel, scale),
        out_shape=(pltpu.VMEM((16, 64, 256), F32), pltpu.VMEM((16, 2, 256), F32)),
        in_specs=[anywhere, anywhere, anywhere],
        out_specs=(vmem, vmem),
        scratch_shapes=[
            vm(slab.shape, F32), vm((16, 16), jnp.int32), vm((NY, 16, 256), F32), vm((4, 8, 128), F32),
            vm((4, 1, 128), jnp.int32), vm((16, 1, 128), jnp.int32), vm((4, 8, 1, 128), jnp.int32),
            pltpu.SMEM((16, 1, 128), jnp.int32), pltpu.SMEM((4, 8, 1, 128), jnp.int32), vm((2, 1, 128), jnp.int32), pltpu.SMEM((2, 1, 128), jnp.int32),
            *[vm((4, 8, HALF, n, 128), F32) for _ in range(4) for n in sizes],
            *[vm((NZ, NC, NX, CAP, n, 128), F32) for n in sizes],
            *[vm((3, 64, n, 128), F32) for n in sizes],
            *[vm((NY, 64, n, 128), F32) for n in sizes],
            vm((4, 256, 256), F32), vm((4, 256, 128), F32), vm((4, 256, 128), F32),
            vm((4, 256, 256), F32), vm((4, 2, 256), F32),
            *[dma(()) for _ in range(13)], dma((NCH,)), dma(()), dma((NCH,)), dma(()), dma((NCH,)), dma((4,)), *[dma(()) for _ in range(4)],
        ],
        compiler_params=pltpu.CompilerParams(collective_id=0, has_side_effects=True, vmem_limit_bytes=58 * 2**20),
    )(ids, query, slab)


def per_device(slab, queries, block_ids):
    query_count, width_part = queries.shape
    full_width = width_part * lax.axis_size("pb")
    blocks_each = slab.shape[0] // BLOCK
    part, vec = main_call(math.sqrt(full_width), block_ids, queries, slab.reshape(blocks_each, BLOCK, width_part))
    own = lax.dynamic_slice_in_dim(vec, lax.axis_index("pb") * 64, 64, 2)
    scores = vec[:, 0]
    gram = part * (own[:, 1][:, :, None] * vec[:, 1][:, None, :])
    penalty = gram * jax.nn.sigmoid(scores[:, None, :] - own[:, 0][:, :, None])
    return (scores, gram, penalty)


def solution(mesh):
    return jax.shard_map(
        per_device,
        mesh=mesh,
        in_specs=(P("db", "pb"), P("db", "pb"), P("db", None)),
        out_specs=(P("db", None), P("db", "pb", None), P("db", "pb", None)),
        check_vma=False,
    )
```
